16 devices in a mesh: dp: 16 (over z, y, x, core).
Axes of the slice: x: 2, y: 2, z: 2, core: 2. Of those that a mesh axis runs over, the one named last changes fastest.
Arguments:
- x_saved: bfloat16 [32, 768, 1536], P('dp')
- grad_out: bfloat16 [32, 768, 1536], P('dp')
- positions: int32 [32, 768], P('dp')
- attn_gain: bfloat16 [1536], replicated
- w_query: bfloat16 [1536, 12, 128], replicated
- w_key: bfloat16 [1536, 2, 128], replicated
- w_value: bfloat16 [1536, 2, 128], replicated
- w_out: bfloat16 [12, 128, 1536], replicated
- mlp_gain: bfloat16 [1536], replicated
- w_gate: bfloat16 [1536, 8960], replicated
- w_up: bfloat16 [1536, 8960], replicated
- w_down: bfloat16 [8960, 1536], replicated
- master_flat: float32 [46795776], P('dp')
- adam_mean: float32 [46795776], P('dp')
- adam_var: float32 [46795776], P('dp')
Outputs:
- output 1: bfloat16 [32, 768, 1536], P('dp')
- output 2: bfloat16 [1536], replicated
- output 3: bfloat16 [1536, 12, 128], replicated
- output 4: bfloat16 [1536, 2, 128], replicated
- output 5: bfloat16 [1536, 2, 128], replicated
- output 6: bfloat16 [12, 128, 1536], replicated
- output 7: bfloat16 [1536], replicated
- output 8: bfloat16 [1536, 8960], replicated
- output 9: bfloat16 [1536, 8960], replicated
- output 10: bfloat16 [8960, 1536], replicated
- output 11: float32 [46795776], P('dp')
- output 12: float32 [46795776], P('dp')
- output 13: float32 [46795776], P('dp')
- output 14: float32 [], replicated
All inputs are finite; a program needn't handle non-finite values.
Results may differ from the reference program's by a relative error of at most 0.0134382.
Values are sent between devices in bfloat16 or wider.
A program may use at most 1.25 GiB of HBM per device.

```python
import math
import jax
import jax.numpy as jnp
from jax import lax

MODEL_DIM = 1536
NUM_HEADS = 12
KV_HEADS = 2
HEAD_DIM = 128
FFN_DIM = 8960
SEQ_LEN = 768
SEQS_DEV = 2
DP_SIZE = 16
STEP_COUNT = 100
TOTAL_SEQS = SEQS_DEV * DP_SIZE
NPARAM = MODEL_DIM * (2 + 2 * HEAD_DIM * (NUM_HEADS + KV_HEADS) + 3 * FFN_DIM)
NORM_EPS = 1e-5
ROPE_BASE = 10000.0
LEARN_RATE = 2e-3
BETA_ONE = 0.9
BETA_TWO = 0.95
ADAM_EPS = 1e-8
WEIGHT_DECAY = 0.1


def param_shapes():
    return [(MODEL_DIM,), (MODEL_DIM, NUM_HEADS, HEAD_DIM), (MODEL_DIM, KV_HEADS, HEAD_DIM),
            (MODEL_DIM, KV_HEADS, HEAD_DIM), (NUM_HEADS, HEAD_DIM, MODEL_DIM), (MODEL_DIM,),
            (MODEL_DIM, FFN_DIM), (MODEL_DIM, FFN_DIM), (FFN_DIM, MODEL_DIM)]


def draw_params(key):
    key_list = jax.random.split(key, 9)
    fan_ins = [0, MODEL_DIM, MODEL_DIM, MODEL_DIM, NUM_HEADS * HEAD_DIM, 0, MODEL_DIM, MODEL_DIM, FFN_DIM]
    drawn_list = []
    for number, piece_shape in enumerate(param_shapes()):
        noise_arr = jax.random.normal(key_list[number], piece_shape, jnp.float32)
        if fan_ins[number] == 0:
            drawn_list.append(1.0 + 0.2 * noise_arr)
        else:
            drawn_list.append(noise_arr * fan_ins[number] ** -0.5)
    return drawn_list


def setup_inputs(seed: int = 0) -> dict:
    key_list = jax.random.split(jax.random.key(seed), 8)
    act_shape = (TOTAL_SEQS, SEQ_LEN, MODEL_DIM)
    x_saved = jax.random.normal(key_list[0], act_shape, jnp.float32).astype(jnp.bfloat16)
    grad_out = jax.random.normal(key_list[1], act_shape, jnp.float32).astype(jnp.bfloat16)
    pos_gaps = jax.random.randint(key_list[2], (TOTAL_SEQS, SEQ_LEN), 1, 4)
    positions = (jnp.cumsum(pos_gaps, axis=1) - 1).astype(jnp.int32)
    weights = [w_piece.astype(jnp.bfloat16) for w_piece in draw_params(key_list[3])]
    master_flat = jnp.concatenate([w_piece.reshape(-1) for w_piece in draw_params(key_list[4])])
    state_scale = NPARAM ** -0.5
    adam_mean = 0.1 * state_scale * jax.random.normal(key_list[5], (NPARAM,), jnp.float32)
    var_root = 0.3 * state_scale * jax.random.uniform(key_list[6], (NPARAM,), jnp.float32, 0.5, 1.5)
    adam_var = var_root * var_root
    return {'x_saved': x_saved, 'grad_out': grad_out, 'positions': positions,
            'attn_gain': weights[0], 'w_query': weights[1], 'w_key': weights[2], 'w_value': weights[3],
            'w_out': weights[4], 'mlp_gain': weights[5], 'w_gate': weights[6], 'w_up': weights[7],
            'w_down': weights[8], 'master_flat': master_flat, 'adam_mean': adam_mean, 'adam_var': adam_var}


def rms_scale(values, gain):
    wide = values.astype(jnp.float32)
    inv_rms = lax.rsqrt(jnp.mean(wide * wide, axis=-1, keepdims=True) + NORM_EPS)
    return (wide * inv_rms * gain.astype(jnp.float32)).astype(jnp.bfloat16)


def rope_tables(positions, head_dim):
    half_dim = head_dim // 2
    inv_freq = ROPE_BASE ** (-2.0 * jnp.arange(half_dim, dtype=jnp.float32) / head_dim)
    angles = positions.astype(jnp.float32)[:, :, None] * inv_freq
    cos_full = jnp.concatenate([jnp.cos(angles), jnp.cos(angles)], axis=-1)[:, :, None, :]
    sin_full = jnp.concatenate([jnp.sin(angles), jnp.sin(angles)], axis=-1)[:, :, None, :]
    return cos_full, sin_full


def rope_apply(values, cos_full, sin_full):
    half_dim = values.shape[-1] // 2
    rotated = jnp.concatenate([-values[..., half_dim:], values[..., :half_dim]], axis=-1)
    return values * cos_full + rotated * sin_full


def layer_forward(w_list, x_val, positions):
    attn_gain, w_query, w_key, w_value, w_out, mlp_gain, w_gate, w_up, w_down = w_list
    num_seqs, seq_len, model_dim = x_val.shape
    num_heads, head_dim = w_query.shape[1], w_query.shape[2]
    kv_heads = w_key.shape[1]
    group_size = num_heads // kv_heads
    n_tok = num_seqs * seq_len
    x_flat = x_val.reshape(n_tok, model_dim)
    normed = rms_scale(x_flat, attn_gain)
    q_pre = jnp.dot(normed, w_query.reshape(model_dim, num_heads * head_dim), preferred_element_type=jnp.float32)
    k_pre = jnp.dot(normed, w_key.reshape(model_dim, kv_heads * head_dim), preferred_element_type=jnp.float32)
    v_pre = jnp.dot(normed, w_value.reshape(model_dim, kv_heads * head_dim), preferred_element_type=jnp.float32)
    v_heads = v_pre.astype(jnp.bfloat16).reshape(num_seqs, seq_len, kv_heads, head_dim)
    cos_full, sin_full = rope_tables(positions, head_dim)
    q_rot = rope_apply(q_pre.reshape(num_seqs, seq_len, num_heads, head_dim), cos_full, sin_full).astype(jnp.bfloat16)
    q_rot = q_rot.reshape(num_seqs, seq_len, kv_heads, group_size, head_dim)
    k_rot = rope_apply(k_pre.reshape(num_seqs, seq_len, kv_heads, head_dim), cos_full, sin_full).astype(jnp.bfloat16)
    scores = jnp.einsum('bqkgd,bskd->bkgqs', q_rot.astype(jnp.float32), k_rot.astype(jnp.float32)) * head_dim ** -0.5
    causal = jnp.arange(seq_len)[:, None] >= jnp.arange(seq_len)[None, :]
    attn_probs = jax.nn.softmax(jnp.where(causal, scores, -1e30), axis=-1).astype(jnp.bfloat16)
    context = jnp.einsum('bkgqs,bskd->bqkgd', attn_probs.astype(jnp.float32), v_heads.astype(jnp.float32)).astype(jnp.bfloat16)
    attn_out = jnp.dot(context.reshape(n_tok, num_heads * head_dim), w_out.reshape(num_heads * head_dim, model_dim), preferred_element_type=jnp.float32)
    hidden = (x_flat.astype(jnp.float32) + attn_out).astype(jnp.bfloat16)
    normed_mlp = rms_scale(hidden, mlp_gain)
    gate_pre = jnp.dot(normed_mlp, w_gate, preferred_element_type=jnp.float32)
    up_pre = jnp.dot(normed_mlp, w_up, preferred_element_type=jnp.float32)
    gated_act = (jax.nn.silu(gate_pre) * up_pre).astype(jnp.bfloat16)
    down_out = jnp.dot(gated_act, w_down, preferred_element_type=jnp.float32)
    return (hidden.astype(jnp.float32) + down_out).astype(jnp.bfloat16).reshape(num_seqs, seq_len, model_dim)


def split_flat(flat_vec):
    pieces = []
    offset = 0
    for piece_shape in param_shapes():
        piece_size = math.prod(piece_shape)
        pieces.append(flat_vec[offset:offset + piece_size].reshape(piece_shape))
        offset += piece_size
    return pieces


def reference(x_saved, grad_out, positions, attn_gain, w_query, w_key, w_value, w_out, mlp_gain, w_gate, w_up, w_down, master_flat, adam_mean, adam_var):
    w_list = (attn_gain, w_query, w_key, w_value, w_out, mlp_gain, w_gate, w_up, w_down)

    def device_grads(grad_acc, group_in):
        x_group, dy_group, pos_group = group_in
        layer_out, pullback = jax.vjp(lambda x_val, w_vals: layer_forward(w_vals, x_val, pos_group), x_group, w_list)
        grad_x, grad_w = pullback(dy_group)
        flat_grad = jnp.concatenate([w_grad.astype(jnp.bfloat16).reshape(-1).astype(jnp.float32) for w_grad in grad_w])
        return grad_acc + flat_grad, grad_x.astype(jnp.bfloat16)

    group_shape = (DP_SIZE, SEQS_DEV, SEQ_LEN, MODEL_DIM)
    grad_sum, grad_x = lax.scan(device_grads, jnp.zeros((NPARAM,), jnp.float32),
                                (x_saved.reshape(group_shape), grad_out.reshape(group_shape),
                                 positions.reshape(DP_SIZE, SEQS_DEV, SEQ_LEN)))
    grad_mean = grad_sum / DP_SIZE
    grad_norm = jnp.sqrt(jnp.sum(grad_mean * grad_mean))
    clip_scale = jnp.minimum(1.0, 1.0 / (grad_norm + 1e-6))
    clipped = grad_mean * clip_scale
    new_mean = BETA_ONE * adam_mean + (1.0 - BETA_ONE) * clipped
    new_var = BETA_TWO * adam_var + (1.0 - BETA_TWO) * clipped * clipped
    mean_hat = new_mean / (1.0 - BETA_ONE ** STEP_COUNT)
    var_hat = new_var / (1.0 - BETA_TWO ** STEP_COUNT)
    gain_two = MODEL_DIM + 2 * MODEL_DIM * HEAD_DIM * (NUM_HEADS + KV_HEADS)
    flat_index = jnp.arange(NPARAM)
    is_gain = (flat_index < MODEL_DIM) | ((flat_index >= gain_two) & (flat_index < gain_two + MODEL_DIM))
    decays = jnp.where(is_gain, 0.0, WEIGHT_DECAY)
    new_master = master_flat - LEARN_RATE * (mean_hat / (jnp.sqrt(var_hat) + ADAM_EPS) + decays * master_flat)
    new_weights = split_flat(new_master.astype(jnp.bfloat16))
    return (grad_x.reshape(TOTAL_SEQS, SEQ_LEN, MODEL_DIM), new_weights[0], new_weights[1], new_weights[2],
            new_weights[3], new_weights[4], new_weights[5], new_weights[6], new_weights[7], new_weights[8],
            new_master, new_mean, new_var, grad_norm)
```

```python
import functools

import jax
import jax.numpy as jnp
import numpy as np
from jax import lax
from jax.experimental import pallas as pl
from jax.experimental.pallas import tpu as pltpu
from jax.sharding import PartitionSpec as P

NORM_EPS = 1e-5
ROPE_BASE = 10000.0
LEARN_RATE = 2e-3
BETA_ONE = 0.9
BETA_TWO = 0.95
ADAM_EPS = 1e-8
WEIGHT_DECAY = 0.1
STEP_COUNT = 100
BF = jnp.bfloat16
F32 = jnp.float32
MESH = pl.DeviceIdType.MESH
LANES = 128
SUB = 16
TILE = 256
HALF_LANES = LANES // 2
DIM = 1536
HEADS = 12
KV_HEADS = 2
GROUP = HEADS // KV_HEADS
KV_DIM = KV_HEADS * LANES
QKV_DIM = DIM + 2 * KV_DIM
FFN = 8960
SEQ = 768
TOK = 2 * SEQ
NDEV = 16
HALF = NDEV // 2
BLK = DIM // NDEV
NPARAM = 46795776
SHARD = NPARAM // NDEV
COLS = FFN // LANES
PER = DIM // LANES
ATTN_ROWS = PER * (2 + 2 * DIM) + 2 * KV_HEADS * DIM
SLAB = BLK * COLS
SLOTS = 5
DOWN_ROWS = FFN // NDEV // SLOTS
BLOCK = 22856
WINDOW = 22880
SCALE = LANES**-0.5
LOG2_E = float(np.log2(np.e))
HBM = pl.BlockSpec(memory_space=pl.ANY)

HOLDERS = "1b028a37945dc6fe" + "6745e81d9c0a2fb3" + "23b95c081da7ef46"
SLAB_DEV = [int(c, NDEV) for c in HOLDERS]
ORDER = [[SLAB_DEV[w * NDEV : (w + 1) * NDEV].index(d) for d in range(NDEV)] for w in range(3)]
SAME = list(range(NDEV))

PLAN = {
    "ffn": ("0259bb", "148abb"),
    "wgrad": ("136777",),
    "dn": ("138bdr", "25cegi", "48fhjr", "lmoqrr"),
    "attn_bwd": ("1258ab", "2369bb", "247abb"),
    "dx": ("1245",),
}


def mm(a, b):
    return jnp.dot(a, b, preferred_element_type=F32)


def mm_nt(a, b):
    return lax.dot_general(a, b, (((1,), (1,)), ((), ())), preferred_element_type=F32)


def mm_tn(a, b):
    return lax.dot_general(a, b, (((0,), (0,)), ((), ())), preferred_element_type=F32)


def step(c):
    return int(c, 36)


def once(i):
    return pl.when(i == 0)


def row_mean(x):
    return jnp.mean(x, axis=-1, keepdims=True)


def row_sum(x):
    return jnp.sum(x, axis=-1, keepdims=True)


def inv_rms(x):
    return lax.rsqrt(row_mean(x * x) + NORM_EPS)


def spec(shape, index, first=0):
    return pl.BlockSpec(shape, lambda *g: tuple(0 if c == "." else g["ijk".index(c)] + first for c in index))


def full(shape):
    return pl.BlockSpec(shape, lambda *_: (0,) * len(shape), pipeline_mode=pl.Buffered(1))


def bf(*shapes):
    return [jax.ShapeDtypeStruct(s, BF) for s in shapes]


def f32(*shapes):
    return [jax.ShapeDtypeStruct(s, F32) for s in shapes]


def dma(*shape):
    return pltpu.SemaphoreType.DMA(shape)


def pcall(kernel, *, grid, in_specs, out_specs, out_shape, name, scratch=(), carry=(), cid=None):
    carry = list(carry or ())
    head, skip = len(in_specs), len(carry)

    def body(*refs):
        kernel(*refs[:head], *refs[head + skip :])

    remote = {} if cid is None else dict(collective_id=cid, has_side_effects=True)
    call = pl.pallas_call(
        body,
        grid=grid,
        in_specs=list(in_specs) + [HBM] * skip,
        out_specs=out_specs,
        scratch_shapes=list(scratch),
        out_shape=out_shape,
        input_output_aliases={head + j: j for j in range(skip)},
        compiler_params=pltpu.CompilerParams(vmem_limit_bytes=63 << 20, **remote),
        cost_estimate=pl.CostEstimate(flops=NPARAM * TILE, bytes_accessed=NPARAM, transcendentals=0),
        name=name,
    )
    return lambda *args: call(*args, *carry)


def flat_slabs(d):
    block = SHARD / LANES
    lo = max(0, int((d * block - ATTN_ROWS) // SLAB))
    hi = int(-(-((d + 1) * block - ATTN_ROWS) // SLAB))
    return list(range(lo, min(hi, 3 * NDEV)))


FLAT_SLABS = [flat_slabs(d) for d in range(NDEV)]


def pick(table, me):
    value = jnp.int32(table[0])
    for d in SAME[1:]:
        value = jnp.where(me == d, jnp.int32(table[d]), value)
    return value


AXES = [[(g + s) % 3 for s in range(3)] for g in range(3)]
LOCAL, FINAL, NSEM = range(10, 13)


def remote_copy(src, dst, send, recv, device):
    return pltpu.make_async_remote_copy(src, dst, send, recv, device_id=(device,), device_id_type=MESH)


class Scatter:
    def __init__(self, a, out, bufs, n, width, sq, row0=0):
        self.a, self.out, self.n, self.sq, self.rows = a, out, n, sq, pl.ds(row0, n)
        self.keep, *self.got, self.sems = bufs
        chunks = width // LANES
        ends = [chunks * g // 3 * LANES for g in range(4)]
        self.cols = [pl.ds(lo, hi - lo) for lo, hi in zip(ends, ends[1:])]
        self.me = lax.axis_index("dp")
        self.chip = self.me // 2
        self.bits = [lax.rem(self.chip // (1 << b), 2) for b in range(3)]

    @staticmethod
    def scratch(n, width):
        return [pltpu.VMEM((k, n, width), BF) for k in (HALF, HALF, 4, 2, 1)] + [dma(2, NSEM)]

    def remote(self, src, dst, k, device):
        return remote_copy(src, dst, self.sems.at[0, k], self.sems.at[1, k], device)

    def whole(self, stage, g):
        ref = self.got[stage + 1].at[:, :, self.cols[g]]
        return self.remote(ref, ref, 1 + 3 * stage + g, self.me ^ 1)

    def loads(self):
        for k, dst in enumerate((self.keep, self.got[0])):
            yield pltpu.make_async_copy(self.a[k].at[:, self.rows, :], dst, self.sems.at[k, LOCAL])

    def start(self):
        for copy in self.loads():
            copy.start()

    def block(self, g, stage, t, send):
        axes = AXES[g]
        own = self.bits[axes[stage]]
        j = (1 - own if send else own) * (1 << axes[stage])
        for s in axes[:stage]:
            j += self.bits[s] * (1 << s)
        for r, s in enumerate(axes[stage + 1 :]):
            j += ((t >> r) & 1) * (1 << s)
        return j

    def push(self, stage):
        for g, axes in enumerate(AXES):
            for t in range(4 >> stage):
                src = self.keep.at[self.block(g, stage, t, True), :, self.cols[g]]
                dst = self.got[stage + 1].at[t, :, self.cols[g]]
                self.remote(src, dst, 1 + 3 * stage + g, self.me ^ (2 << axes[stage])).start()

    def sum_rows(self, j, src, cols):
        def body(r, _):
            sl = pl.ds(pl.multiple_of(r * SUB, SUB), SUB)
            self.keep[j, sl, cols] = self.keep[j, sl, cols] + src[sl, cols]
            return 0

        lax.fori_loop(0, self.n // SUB, body, 0)

    def first(self):
        for copy in self.loads():
            copy.wait()

        def body(j, _):
            self.sum_rows(j, self.got[0].at[j], slice(None))
            return 0

        lax.fori_loop(0, HALF, body, 0)
        self.push(0)

    def merge(self, stage):
        for g in range(3):
            self.whole(stage, g).wait_recv()
            for t in range(4 >> stage):
                self.sum_rows(self.block(g, stage, t, False), self.got[stage + 1].at[t], self.cols[g])
        if stage < 2:
            self.push(stage + 1)

    def hand_over(self):
        return pltpu.make_async_copy(self.keep.at[self.chip], self.out, self.sems.at[0, FINAL])

    def last(self):
        self.merge(2)
        self.hand_over().start()

        def body(r, _):
            g = self.keep[self.chip, pl.ds(pl.multiple_of(r * SUB, SUB), SUB), :].astype(F32) * (1.0 / NDEV)
            g = g * g
            total = g[: SUB // 2] + g[SUB // 2 :]
            for c in range(0, total.shape[1], LANES):
                self.sq[:] += total[:, c : c + LANES]
            return 0

        lax.fori_loop(0, self.n // SUB, body, 0)

    def finish(self):
        self.hand_over().wait()
        for stage in range(3):
            for g in range(3):
                self.whole(stage, g).wait_send()

    def run(self, i, at, final=NPARAM):
        stages = (self.start, self.first, *(functools.partial(self.merge, s) for s in range(2)), self.last, self.finish)
        for c, todo in zip(at, stages):
            k = min(step(c), final)
            if isinstance(i, int):
                if i == k:
                    todo()
            else:
                pl.when(i == k)(todo)

    def hand_on(self, sem):
        for k in (1, 2, 4, 8):
            pl.semaphore_signal(sem, inc=1, device_id=(self.me ^ k,), device_id_type=MESH)


class Push:
    def __init__(self, src, got, sems, weight):
        self.src, self.got, self.sems, self.weight = src, got, sems, weight
        self.me = lax.axis_index("dp")

    def each(self):
        held = [self.weight * NDEV + b for b in ORDER[self.weight]]
        for k in range(2):
            own = [([d for d in SAME if h in FLAT_SLABS[d]][k:] or [-1])[0] for h in held]
            slot = [FLAT_SLABS[d].index(h) if d >= 0 else 0 for d, h in zip(own, held)]
            to, slot = pick(own, self.me), pick(slot, self.me)
            dst, recv = self.got.at[slot], self.sems.at[1, slot]
            there = remote_copy(self.src, dst, self.sems.at[0, k], recv, jnp.maximum(to, 0))
            yield to, pltpu.make_async_copy(self.src, dst, recv), there

    def start(self):
        for to, here, there in self.each():
            pl.when(to == self.me)(here.start)
            pl.when((to >= 0) & (to != self.me))(there.start)

    def finish(self):
        for to, _, there in self.each():
            pl.when((to >= 0) & (to != self.me))(there.wait_send)
        for j in range(SLOTS):
            gets = [len(s) > j and s[j] // NDEV == self.weight for s in FLAT_SLABS]
            pl.when(pick(gets, self.me) == 1)(pltpu.make_async_copy(self.src, self.got.at[j], self.sems.at[1, j]).wait)


def push_all(refs, weights, start):
    n = len(weights)
    for j, w in enumerate(weights):
        job = Push(*refs[j::n], w)
        (job.start if start else job.finish)()


SLOT_SEMS = dma(2, SLOTS)


def push_shapes(parts):
    return bf(*((SLOTS, *p.shape) for p, _ in parts))


def push_sems(parts):
    return [SLOT_SEMS] * len(parts)


def greet():
    me = lax.axis_index("dp")
    for k in SAME[1:]:
        pl.semaphore_signal(pltpu.get_barrier_semaphore(), inc=1, device_id=(me ^ k,), device_id_type=MESH)


def met():
    pl.semaphore_wait(pltpu.get_barrier_semaphore(), NDEV - 1)


SQ_SPEC = full((SUB // 2, LANES))
SQ = f32((SUB // 2, LANES))


def blocks(pairs):
    return [g.reshape(HALF, -1, g.shape[-1]) for pair in pairs for g in pair]


def row_block(order, p, core):
    j, mine = 2 * (p % HALF), p // HALF
    return jnp.where(core == mine, order[j + 1], order[j])


def head_pair(w_ref, h):
    return jnp.concatenate([w_ref[h], w_ref[h + 1]], axis=1)


def qkv_kernel(x_ref, g_ref, wq_ref, wk_ref, wv_ref, c_ref, s_ref, nt_ref, q_ref, k_ref, v_ref):
    x = x_ref[:].astype(F32)
    inv = inv_rms(x)
    n = (x * inv * g_ref[:]).astype(BF)
    nt_ref[:] = n.T
    c, s = c_ref[:], s_ref[:]

    def rope(out, t, h):
        for j in range(2):
            u = t[:, j * LANES : (j + 1) * LANES]
            cols = slice((h + j) * LANES, (h + j + 1) * LANES)
            out[:, cols] = (u * c + pltpu.roll(u, HALF_LANES, 1) * s).astype(BF)

    for h in range(0, HEADS, 2):
        rope(q_ref, mm(n, head_pair(wq_ref, h)), h)
    rope(k_ref, mm(n, wk_ref[:]), 0)
    v_ref[:] = mm(n, wv_ref[:]).astype(BF)


def qkv_call(x, gain, wq, wk, wv, cos, sin, tile=TILE):
    r = lambda w: spec((tile, w), "i.")
    return pcall(
        qkv_kernel,
        grid=(TOK // tile,),
        in_specs=[r(DIM), full(gain.shape), full(wq.shape), full(wk.shape), full(wv.shape), r(LANES), r(LANES)],
        out_specs=[spec((DIM, tile), ".i"), r(DIM), r(KV_DIM), r(KV_DIM)],
        out_shape=bf((DIM, TOK), (TOK, DIM), (TOK, KV_DIM), (TOK, KV_DIM)),
        name="qkv",
    )(x, gain, wq, wk, wv, cos, sin)


def probs(q, k, i, bq):
    s = mm_nt(q, k[: (i + 1) * bq])
    r = lax.broadcasted_iota(jnp.int32, (bq, bq), 0)
    c = lax.broadcasted_iota(jnp.int32, (bq, bq), 1)
    d = jnp.where(r >= c, s[:, i * bq :], -1e30)
    s = jnp.concatenate([s[:, : i * bq], d], axis=1) if i else d
    e = jnp.exp2((s - jnp.max(s, axis=-1, keepdims=True)) * (SCALE * LOG2_E))
    return e * (1.0 / row_sum(e))


def head_cols(h):
    return slice(h * LANES, (h + 1) * LANES)


def attn_fwd_kernel(q_ref, k_ref, v_ref, o_ref, ot_ref, *, bq):
    k, v = k_ref[:], v_ref[:]
    for i in range(SEQ // bq):
        r = slice(i * bq, (i + 1) * bq)
        for c in map(head_cols, range(GROUP)):
            p = probs(q_ref[r, c], k, i, bq).astype(BF)
            o = mm(p, v[: (i + 1) * bq]).astype(BF)
            o_ref[r, c] = o
            ot_ref[c, r] = o.T


def attn_fwd(q, k, v, bq=384):
    hq, hk = spec((SEQ, GROUP * LANES), "ij"), spec((SEQ, LANES), "ij")
    return pcall(
        functools.partial(attn_fwd_kernel, bq=bq),
        grid=(TOK // SEQ, KV_HEADS),
        in_specs=[hq, hk, hk],
        out_specs=[hq, spec((GROUP * LANES, SEQ), "ji")],
        out_shape=bf((TOK, DIM), (DIM, TOK)),
        name="attn_fwd",
    )(q, k, v)


def attn_bwd_kernel(q_ref, k_ref, v_ref, do_ref, c_ref, s_ref, out_k, out_r, down_k, down_r, *refs, weights, bq, nh):
    nw = len(weights)
    ins, (dq_ref, dk_ref, dv_ref, out_out, down_a, down_b), refs = refs[:nw], refs[nw:][:6], refs[nw + 6 :]
    gots, (sq, dka, dva), sems, refs = refs[:nw], refs[nw:][:3], refs[nw + 3 :][:nw], refs[2 * nw + 3 :]
    pushes = (*ins, *gots, *sems)
    b, kv, group = (pl.program_id(j) for j in range(3))
    steps = GROUP // nh
    i = (b * KV_HEADS + kv) * steps + group
    n = DOWN_ROWS

    @once(i)
    def _():
        sq[:] = jnp.zeros_like(sq)
        greet()

    @pl.when(i == 1)
    def _():
        met()
        push_all(pushes, weights, True)

    down, plan = (down_k, down_r), PLAN["attn_bwd"]
    Scatter(down, down_a, refs[:6], n, DIM, sq, 3 * n).run(i, plan[0])
    Scatter(down, down_b, refs[6:12], n, DIM, sq, 4 * n).run(i, plan[1])
    Scatter((out_k, out_r), out_out, refs[12:], BLK, DIM, sq).run(i, plan[2])
    pl.when(i == step(plan[0][-1]))(lambda: push_all(pushes, weights, False))
    k, v = k_ref[:], v_ref[:]

    @once(group)
    def _():
        dka[:] = jnp.zeros_like(dka)
        dva[:] = jnp.zeros_like(dva)

    def back(t, c, s):
        return (t * c - pltpu.roll(t, HALF_LANES, 1) * s).astype(BF)

    for i in range(SEQ // bq):
        r, w = slice(i * bq, (i + 1) * bq), (i + 1) * bq
        sides = [[], [], [], []]
        for c in map(head_cols, range(nh)):
            q, do = q_ref[r, c], do_ref[r, c]
            p = probs(q, k, i, bq)
            dp = mm_nt(do, v[:w])
            ds = (p * (dp - row_sum(dp * p)) * SCALE).astype(BF)
            dq_ref[r, c] = back(mm(ds, k[:w]), c_ref[r, :], s_ref[r, :])
            for side, value in zip(sides, (ds, q, p.astype(BF), do)):
                side.append(value)
        ds, q, p, do = (jnp.concatenate(side, axis=0) for side in sides)
        dka[:w, :] += mm_tn(ds, q)
        dva[:w, :] += mm_tn(p, do)

    @pl.when(group == steps - 1)
    def _():
        dk_ref[:] = back(dka[:], c_ref[:], s_ref[:])
        dv_ref[:] = dva[:].astype(BF)


def attn_bwd(q, k, v, do, cos, sin, g_out, g_down, parts, cid, bq=384, nh=2):
    steps = GROUP // nh
    hq = pl.BlockSpec((SEQ, nh * LANES), lambda b, kv, g: (b, kv * steps + g))
    hk = spec((SEQ, LANES), "ij")
    tb = spec((SEQ, LANES), "i.")
    down = (DOWN_ROWS, DIM)
    return pcall(
        functools.partial(attn_bwd_kernel, weights=[w for _, w in parts], bq=bq, nh=nh),
        grid=(TOK // SEQ, KV_HEADS, steps),
        in_specs=[hq, hk, hk, hq, tb, tb] + [HBM] * (4 + len(parts)),
        out_specs=[hq, hk, hk] + [HBM] * (3 + len(parts)) + [SQ_SPEC],
        out_shape=bf((TOK, DIM), k.shape, v.shape, (BLK, DIM), down, down) + push_shapes(parts) + SQ,
        scratch=[pltpu.VMEM((SEQ, LANES), F32)] * 2
        + push_sems(parts)
        + Scatter.scratch(*down) * 2
        + Scatter.scratch(BLK, DIM),
        name="attn_bwd",
        cid=cid,
    )(q, k, v, do, cos, sin, *blocks([g_out, g_down]), *[p for p, _ in parts])


def oproj_kernel(c_ref, wo_ref, x_ref, g_ref, h_ref, n_ref, nt_ref):
    h = (x_ref[:].astype(F32) + mm(c_ref[:], wo_ref[:])).astype(BF)
    h_ref[:] = h
    hw = h.astype(F32)
    inv = inv_rms(hw)
    n = (hw * inv * g_ref[:]).astype(BF)
    n_ref[:] = n
    nt_ref[:] = n.T


def oproj_call(ctx, wo, x, gain, tile=TILE):
    r = spec((tile, DIM), "i.")
    return pcall(
        oproj_kernel,
        grid=(TOK // tile,),
        in_specs=[r, full(wo.shape), r, full(gain.shape)],
        out_specs=[r, r, spec((DIM, tile), ".i")],
        out_shape=bf((TOK, DIM), (TOK, DIM), (DIM, TOK)),
        name="oproj",
    )(ctx, wo, x, gain)


def ffn_kernel(nm_h, dy_h, nt_h, wg_ref, wu_ref, wd_ref, *refs, units, at, weights, count, rc):
    nu, nw = len(units), len(weights)
    ins, refs = refs[: 2 * nu + nw], refs[2 * nu + nw :]
    (gt_ref, dg_ref, du_ref, gg_ref, gu_ref, rg_h, ru_h), refs = refs[:7], refs[7:]
    outs, (sq, nm, dy, na, nb, out, sem, core_sem), refs = refs[: nu + nw], refs[nu + nw :][:8], refs[nu + nw + 8 :]
    pushes = (*ins[2 * nu :], *outs[nu:], *refs[:nw])
    i = pl.program_id(0)
    me = lax.axis_index("dp")
    half, tile = out.shape[-2:]
    loads = [(nm_h, nm), (dy_h, dy), (nt_h, na), (nt_h, nb)]

    @once(i)
    def _():
        sq[:] = jnp.zeros_like(sq)
        for j, (src, dst) in enumerate(loads):
            if src is not nt_h:
                pltpu.make_async_copy(src, dst, sem.at[j]).start()
                continue
            for p in range(NDEV):
                b = row_block(ORDER[j - 2], p, lax.rem(me, 2))
                rows = src.at[pl.ds(pl.multiple_of(b * BLK, BLK), BLK)]
                pltpu.make_async_copy(rows, dst.at[pl.ds(p * BLK, BLK)], sem.at[j]).start()
        greet()

    jobs = [
        Scatter(ins[2 * u :][:2], outs[u], refs[nw + 6 * u :][:6], *unit, sq) for u, unit in enumerate(units)
    ]

    @once(i)
    def _():
        for j, (src, dst) in enumerate(loads):
            pltpu.make_async_copy(src, dst, sem.at[j]).wait()

    slot = lax.rem(i, 2)

    def across(w, dst, t):
        cols = dst.at[:, pl.ds(pl.multiple_of(t * tile, tile), tile)]
        slot = lax.rem(t, 2)
        return remote_copy(out.at[slot, w], cols, core_sem.at[slot, w], core_sem.at[2, w], me ^ 1)

    @pl.when(i >= 2)
    def _():
        for w, dst in enumerate((rg_h, ru_h)):
            across(w, dst, i - 2).wait_send()

    for r in range(0, TOK, rc):
        sl = pl.ds(r, rc)
        gate = mm(nm[sl, :], wg_ref[:])
        up = mm(nm[sl, :], wu_ref[:])
        dga = mm_nt(dy[sl, :], wd_ref[:])
        sig = 1.0 / (1.0 + jnp.exp(-gate))
        act = gate * sig
        gt_ref[:, sl] = (act * up).astype(BF).T
        du_ref[sl, :] = (dga * act).astype(BF)
        dg_ref[sl, :] = (dga * up * sig * (1.0 + gate * (1.0 - sig))).astype(BF)

    @once(i)
    def _():
        met()
        push_all(pushes, weights, True)

    for job, when in zip(jobs, at):
        job.run(i, when, count - 1)
    if nw:
        pl.when(i == count - 1)(lambda: push_all(pushes, weights, False))
    for w, (src, rhs, keep) in enumerate(((na, dg_ref, gg_ref), (nb, du_ref, gu_ref))):
        out[slot, w] = mm(src[:half, :], rhs[:]).astype(BF)
        keep[:] = mm(src[half:, :], rhs[:]).astype(BF)
    for w, dst in enumerate((rg_h, ru_h)):
        across(w, dst, i).start()

        @pl.when(i == count - 1)
        def _(w=w, dst=dst):
            across(w, dst, i - 1).wait_send()
            across(w, dst, i).wait_send()
            remote_copy(dst, dst, core_sem.at[0, w], core_sem.at[2, w], me ^ 1).wait_recv()


def ffn_slice(nm, dy, nt, wg, wu, wd, first, count, prev, arrays, at, parts, cid, tile=TILE, rc=TILE):
    width, half = count * tile, DIM // 2
    units = [(BLK, g.shape[-1]) for g, _ in arrays]
    nmore = len(units) + len(parts)
    col, row, grad = spec((DIM, tile), ".i", first), spec((tile, DIM), "i.", first), spec((half, tile), ".i")
    outs = bf((FFN, TOK), (TOK, FFN), (TOK, FFN), *[(half, width)] * 4, *units)
    return pcall(
        functools.partial(ffn_kernel, units=units, at=at, weights=[w for _, w in parts], count=count, rc=rc),
        grid=(count,),
        in_specs=[HBM] * 3 + [col, col, row] + [HBM] * (nmore + len(units)),
        out_specs=[row, col, col, grad, grad] + [HBM] * (2 + nmore) + [SQ_SPEC],
        out_shape=outs + push_shapes(parts) + SQ,
        scratch=[pltpu.VMEM((TOK, DIM), BF)] * 4
        + [pltpu.VMEM((2, 2, half, tile), BF), dma(4), dma(3, 2)]
        + push_sems(parts)
        + [t for u in units for t in Scatter.scratch(*u)],
        name="ffn",
        carry=prev,
        cid=cid,
    )(nm, dy, nt, wg, wu, wd, *blocks(arrays), *[p for p, _ in parts])


def wgrad_kernel(lhs_h, *refs, cols, nr, per, blk, order, units, at, weights):
    nrhs, nu, nw = len(cols), len(units), len(weights)
    nm = nu + nw
    rhs_h, ins, (keep_h, other_h, *refs) = refs[:nrhs], refs[nrhs:][: nm + nu], refs[nrhs + nm + nu :]
    outs, (sq, *refs) = refs[:nm], refs[nm:]
    me = lax.axis_index("dp")
    rhs, (lhs, out, sem_l, sem_r, sem_o), refs = refs[:nrhs], refs[nrhs:][:5], refs[nrhs + 5 :]
    pushes = (*ins[2 * nu :], *outs[nu:], *refs[:nw])
    size = per * nr
    steps = NDEV * blk // size
    ring = lhs.shape[0]

    def fetch(t):
        for j in range(per):
            p, r = divmod((t * per + j) * nr, blk)
            src = lhs_h.at[pl.ds(pl.multiple_of(row_block(order, p, lax.rem(me, 2)) * blk + r, SUB), nr)]
            pltpu.make_async_copy(src, lhs.at[t % ring, pl.ds(j * nr, nr)], sem_l.at[t % ring]).start()

    def rhs_copy(j):
        c, w = cols[j]
        return pltpu.make_async_copy(rhs_h[j].at[:, pl.ds(c, w)], rhs[j], sem_r.at[j])

    def remote(src, dst, slot):
        return remote_copy(src, dst, sem_o.at[slot], sem_o.at[2], me ^ 1)

    def out_copy(t, wait):
        src, slot, half = out.at[t % 2], t % 2, steps // 2
        if t < half:
            copy = remote(src, other_h.at[pl.ds(t * size, size)], slot)
            (copy.wait_send if wait else copy.start)()
        else:
            copy = pltpu.make_async_copy(src, keep_h.at[pl.ds((t - half) * size, size)], sem_o.at[slot])
            (copy.wait if wait else copy.start)()

    fetch(0)
    for j in range(nrhs):
        rhs_copy(j).start()
    fetch(1)
    sq[:] = jnp.zeros_like(sq)
    greet()
    jobs = [Scatter(ins[2 * u :][:2], outs[u], refs[nw + 6 * u :][:6], *unit, sq) for u, unit in enumerate(units)]
    for t in range(steps):
        if t + 2 < steps:
            fetch(t + 2)
        pltpu.make_async_copy(lhs_h.at[pl.ds(0, size)], lhs.at[t % ring], sem_l.at[t % ring]).wait()
        if t >= 2:
            out_copy(t - 2, True)
        c = 0
        for j in range(nrhs):
            if t == 0:
                rhs_copy(j).wait()
            o = mm(lhs[t % ring], rhs[j][:]).astype(BF)
            out[t % 2, :, c : c + o.shape[1]] = o
            c += o.shape[1]
        if t == 0:
            met()
            push_all(pushes, weights, True)
        out_copy(t, False)
        for job in jobs:
            job.run(t, at)
    for t in range(steps - 2, steps):
        out_copy(t, True)
    remote(other_h, other_h, 0).wait_recv()
    push_all(pushes, weights, False)


def wgrad(lhs_t, rhs, nr, per, order, cid, arrays=(), at="", parts=()):
    rows, width = lhs_t.shape[0], sum(w for _, _, w in rhs)
    units = [(BLK, g.shape[-1]) for g, _ in arrays]
    nmore = len(units) + len(parts)
    return pcall(
        functools.partial(
            wgrad_kernel,
            cols=[r[1:] for r in rhs],
            nr=nr,
            per=per,
            blk=rows // NDEV,
            order=order,
            units=units,
            at=at,
            weights=[w for _, w in parts],
        ),
        grid=(1,),
        in_specs=[HBM] * (1 + len(rhs) + nmore + len(units)),
        out_specs=[HBM] * (2 + nmore) + [SQ_SPEC],
        out_shape=bf(*[(rows // 2, width)] * 2, *units) + push_shapes(parts) + SQ,
        scratch=[pltpu.VMEM((TOK, w), BF) for _, _, w in rhs]
        + [pltpu.VMEM((3, per * nr, TOK), BF), pltpu.VMEM((2, per * nr, width), BF), dma(3), dma(len(rhs)), dma(3)]
        + push_sems(parts)
        + [t for u in units for t in Scatter.scratch(*u)],
        name="wgrad",
        cid=cid,
    )(lhs_t, *[r[0] for r in rhs], *blocks(arrays), *[p for p, _ in parts])


def norm_back(d, x, g_ref, gg_ref):
    inv = inv_rms(x)
    hat = x * inv
    gg_ref[:] += jnp.sum(d * hat, axis=0, keepdims=True)
    dg = d * g_ref[:]
    return inv * (dg - hat * row_mean(dg * hat))


def dn_kernel(dg_ref, du_ref, wg_ref, wu_ref, h_ref, dy_ref, g_ref, up_k, up_r, down_k, down_r, part_h, dh_ref, dl_ref, gg_ref, *refs, up):
    up_out, down_a, down_b, down_c, got, sq, acc, ready, psem, *refs = refs
    push = Push(part_h, got, psem, 0)
    t, k = pl.program_id(0), pl.program_id(1)
    i = t * pl.num_programs(1) + k
    n = DOWN_ROWS

    @once(i)
    def _():
        gg_ref[:] = jnp.zeros_like(gg_ref)
        sq[:] = jnp.zeros_like(sq)
        greet()

    @pl.when(i == 1)
    def _():
        met()
        push.start()

    plan = PLAN["dn"]
    up_h, down_h = (up_k, up_r), (down_k, down_r)
    one = Scatter(down_h, down_a, refs[6:12], n, DIM, sq)
    three = Scatter(down_h, down_c, refs[6:11] + refs[18:], n, DIM, sq, 2 * n)
    Scatter(up_h, up_out, refs[:6], *up, sq).run(i, plan[0])
    one.run(i, plan[1])
    Scatter(down_h, down_b, refs[12:18], n, DIM, sq, n).run(i, plan[2])
    pl.when(i == step(plan[1][-1]))(lambda: one.hand_on(ready))
    pl.when(i == step(plan[3][0]))(lambda: pl.semaphore_wait(ready, 4))
    three.run(i, plan[3])
    pl.when(i == step("r"))(push.finish)

    @once(k)
    def _():
        acc[:] = jnp.zeros_like(acc)

    acc[:] += mm_nt(dg_ref[:], wg_ref[:]) + mm_nt(du_ref[:], wu_ref[:])

    @pl.when(k == pl.num_programs(1) - 1)
    def _():
        def body(r, _):
            sl = pl.ds(pl.multiple_of(r * LANES, LANES), LANES)
            o = norm_back(acc[sl, :], h_ref[sl, :].astype(F32), g_ref, gg_ref) + dy_ref[sl, :].astype(F32)
            dh_ref[sl, :] = o
            dl_ref[sl, :] = o.astype(BF)
            return 0

        lax.fori_loop(0, acc.shape[0] // LANES, body, 0)


def dn_call(dg, du, wg, wu, h, dy, gain, g_up, g_down, part, cid, tt=384, tk=1280):
    up, down = (BLK, g_up[0].shape[-1]), (DOWN_ROWS, DIM)
    act, wgt, row = spec((tt, tk), "ij"), spec((DIM, tk), ".j"), spec((tt, DIM), "i.")
    gained = spec(gain.shape, "..")
    return pcall(
        functools.partial(dn_kernel, up=up),
        grid=(TOK // tt, FFN // tk),
        in_specs=[act, act, wgt, wgt, row, row, full(gain.shape)] + [HBM] * 5,
        out_specs=[row, row, gained] + [HBM] * 5 + [SQ_SPEC],
        out_shape=f32((TOK, DIM)) + bf((TOK, DIM)) + f32(gain.shape) + bf(up, *[down] * 3) + push_shapes([(part, 0)]) + SQ,
        scratch=[pltpu.VMEM((tt, DIM), F32), pltpu.SemaphoreType.REGULAR, SLOT_SEMS]
        + Scatter.scratch(*up)
        + Scatter.scratch(*down) * 2
        + Scatter.scratch(*down)[-1:],
        name="dn",
        cid=cid,
    )(dg, du, wg, wu, h, dy, gain, *blocks([g_up, g_down]), part)


def dx_kernel(
    dq_ref, dk_ref, dv_ref, wq_ref, wk_ref, wv_ref, x_ref, g_ref, dh_ref, sq_ref, g_two_ref, qkv_k, qkv_r,
    dx_ref, gg_ref, qkv_out, told_ref, sq, mine, told, tell, *refs,
):
    i = pl.program_id(0)

    @once(i)
    def _():
        gg_ref[:] = jnp.zeros_like(gg_ref)
        sq[:] = sq_ref[:]
        greet()

    pl.when(i == 1)(met)
    scatter = Scatter((qkv_k, qkv_r), qkv_out, refs, BLK, QKV_DIM, sq)
    scatter.run(i, *PLAN["dx"])
    d = mm_nt(dk_ref[:], wk_ref[:]) + mm_nt(dv_ref[:], wv_ref[:])
    for h in range(0, HEADS, 2):
        d += mm_nt(dq_ref[:, h * LANES : (h + 2) * LANES], head_pair(wq_ref, h))
    dx_ref[:] = (norm_back(d, x_ref[:].astype(F32), g_ref, gg_ref) + dh_ref[:]).astype(BF)

    @pl.when(i == pl.num_programs(0) - 1)
    def _():
        scatter.last()
        for row, ref in enumerate((gg_ref, g_two_ref)):
            for c in range(PER):
                mine[pl.ds(row * PER + c, 1), :] = ref[:, head_cols(c)].astype(BF).astype(F32)
        mine[2 * PER :, :] = sq[:]
        me = lax.axis_index("dp")
        copies = []
        for k in SAME[1:]:
            copies.append(remote_copy(mine, told.at[me], tell.at[0, k], tell.at[1, k], me ^ k))
            copies[-1].start()
        told[me] = mine[:]
        for copy in copies:
            copy.wait()
        told_ref[:] = told[:]
        scatter.finish()


def dx_call(dq, dk, dv, wq, wk, wv, x, gain, dh, squares, g_two, g_qkv, cid, tile=TILE):
    r = lambda w: spec((tile, w), "i.")
    told = (2 * PER + squares.shape[0], LANES)
    return pcall(
        dx_kernel,
        grid=(TOK // tile,),
        in_specs=[r(DIM), r(KV_DIM), r(KV_DIM), full(wq.shape), full(wk.shape), full(wv.shape), r(DIM), full(gain.shape)]
        + [r(DIM), SQ_SPEC, full(gain.shape), HBM, HBM],
        out_specs=[r(DIM), spec(gain.shape, ".."), HBM, full((NDEV, *told))],
        out_shape=bf((TOK, DIM)) + f32(gain.shape) + bf((BLK, QKV_DIM)) + f32((NDEV, *told)),
        scratch=[pltpu.VMEM(squares.shape, F32), pltpu.VMEM(told, F32), pltpu.VMEM((NDEV, *told), F32), dma(2, NDEV)] + Scatter.scratch(BLK, QKV_DIM),
        name="dx",
        cid=cid,
    )(dq, dk, dv, wq, wk, wv, x, gain, dh, squares, g_two, *blocks([g_qkv]))


def to_lane_rows(wide, base, per, part, col, rows):
    for j in range(part.shape[1] // LANES):
        piece = part[:, j * LANES : (j + 1) * LANES].astype(F32)
        wide[pl.ds(base + col + j, rows, stride=per), :] = piece


def attn_flat_kernel(x_ref, o_ref, wide, *, segs):
    base = 0
    for col, per in segs:
        to_lane_rows(wide, base, per, x_ref[:, col * LANES : (col + per) * LANES], 0, BLK)
        base += BLK * per
    o_ref[:] = wide[:].astype(BF)


def attn_flat(x, *segs):
    rows = x.size // LANES
    return pcall(
        functools.partial(attn_flat_kernel, segs=segs),
        grid=(1,),
        in_specs=[full(x.shape)],
        out_specs=full((rows, LANES)),
        out_shape=bf((rows, LANES))[0],
        scratch=[pltpu.VMEM((rows, LANES), F32)],
        name="attn_flat",
    )(x)


def collect_kernel(*refs, ng, nd):
    gates, ups, downs = refs[:ng], refs[ng : 2 * ng], refs[2 * ng : 2 * ng + nd]
    o_h, tall, flat, wide, out, sem = refs[2 * ng + nd :]
    me = lax.axis_index("dp")
    kinds = [[s[k] // NDEV if k < len(s) else -1 for s in FLAT_SLABS] for k in range(SLOTS)]

    def copies(k, parts, dst, axis):
        at = 0
        for p in parts:
            n = p.shape[axis]
            to = dst.at[:, pl.ds(at, n)] if axis == 2 else dst.at[pl.ds(at, n)]
            yield pltpu.make_async_copy(p.at[k], to, sem.at[0])
            at += n

    for k in range(SLOTS):
        kind = pick(kinds[k], me)
        for w, parts in enumerate((gates, ups, downs)):

            @pl.when(kind == w)
            def _(k=k, w=w, parts=parts):
                todo = list(copies(k, parts, *((tall, 1) if w == 2 else (flat, 2))))
                for c in todo:
                    c.start()
                for c in todo:
                    c.wait()

        def store(k=k):
            return pltpu.make_async_copy(out, o_h.at[pl.ds(k * SLAB, SLAB)], sem.at[1])

        @pl.when(kind == 2)
        def _():
            to_lane_rows(wide, 0, PER, tall, 0, tall.shape[0])

        @pl.when((kind == 0) | (kind == 1))
        def _():
            to_lane_rows(wide, 0, COLS, flat, 0, BLK)

        if k:
            store(k - 1).wait()
        out[:] = wide[:].astype(BF)
        store().start()
    store().wait()


def collect(gates, ups, downs):
    parts = [*gates, *ups, *downs]
    return pcall(
        functools.partial(collect_kernel, ng=len(gates), nd=len(downs)),
        grid=(1,),
        in_specs=[HBM] * len(parts),
        out_specs=HBM,
        out_shape=bf((SLOTS * SLAB, LANES))[0],
        scratch=[
            pltpu.VMEM((FFN // NDEV, DIM), BF),
            pltpu.VMEM((BLK, FFN), BF),
            pltpu.VMEM((SLAB, LANES), F32),
            pltpu.VMEM((SLAB, LANES), BF),
            dma(2),
        ],
        name="collect",
    )(*parts)


def paste_kernel(*refs, pieces):
    srcs, (o_ref, sem) = refs[:-2], refs[-2:]
    todo = []
    for s, lead, row, n, dst in pieces:
        src = srcs[s] if lead is None else srcs[s].at[lead]
        todo.append(pltpu.make_async_copy(src.at[pl.ds(row, n)], o_ref.at[pl.ds(dst, n)], sem.at[len(todo)]))
    for c in todo:
        c.start()
    for c in todo:
        c.wait()


def paste(srcs, pieces):
    placed, at = [], 0
    for p in pieces:
        placed.append((*p, at))
        at += p[-1]
    return pcall(
        functools.partial(paste_kernel, pieces=placed),
        grid=(1,),
        in_specs=[HBM] * len(srcs),
        out_specs=full((WINDOW, LANES)),
        out_shape=bf((WINDOW, LANES))[0],
        scratch=[dma(len(placed))],
        name="paste",
    )(*srcs)


def unflat_kernel(x_ref, o_ref, wide, *, per, skew, head_major):
    wide[:] = x_ref[:].astype(F32)
    n = (x_ref.shape[0] - SUB * (skew > 0)) // per
    for j in range(per):
        t = wide[pl.ds(j + skew, n, stride=per), :].astype(BF)
        if head_major:
            o_ref[j] = t
        else:
            o_ref[:, j * LANES : (j + 1) * LANES] = t


def unflat(flat, start, rows, per, tile, head_major=False):
    out = (per, rows, LANES) if head_major else (rows, per * LANES)
    skew = start % 8
    n, window = tile * per, tile * per + SUB * (skew > 0)
    source = lambda i: (pl.multiple_of(start - skew + n * i, 8), 0)
    return pcall(
        functools.partial(unflat_kernel, per=per, skew=skew, head_major=head_major),
        grid=(rows // tile,),
        in_specs=[pl.BlockSpec((pl.Element(window), pl.Element(LANES)), source)],
        out_specs=spec((per, tile, LANES), ".i.") if head_major else spec((tile, per * LANES), "i."),
        out_shape=bf(out)[0],
        scratch=[pltpu.VMEM((window, LANES), F32)],
        name="unflat",
    )(flat)


def rope_tables(positions):
    inv_freq = ROPE_BASE ** (-jnp.arange(HALF_LANES, dtype=F32) / HALF_LANES)
    angles = positions.astype(F32).reshape(-1)[:, None] * inv_freq
    cos, sin = jnp.cos(angles), jnp.sin(angles)
    return jnp.concatenate([cos, cos], axis=-1), jnp.concatenate([-sin, sin], axis=-1)


def adamw_apply(grad_vec, grad_norm, master_vec, mean_vec, var_vec, first_index):
    clip_scale = jnp.minimum(1.0, 1.0 / (grad_norm + 1e-6))
    clipped = grad_vec * clip_scale
    new_mean = BETA_ONE * mean_vec + (1.0 - BETA_ONE) * clipped
    new_var = BETA_TWO * var_vec + (1.0 - BETA_TWO) * clipped * clipped
    mean_hat = new_mean / (1.0 - BETA_ONE**STEP_COUNT)
    var_hat = new_var / (1.0 - BETA_TWO**STEP_COUNT)
    flat_index = first_index + lax.iota(jnp.int32, master_vec.shape[0])
    gain_two = ATTN_ROWS * LANES - DIM
    is_gain = (flat_index < DIM) | ((flat_index >= gain_two) & (flat_index < gain_two + DIM))
    decays = jnp.where(is_gain, 0.0, WEIGHT_DECAY)
    new_master = master_vec - LEARN_RATE * (mean_hat / (jnp.sqrt(var_hat) + ADAM_EPS) + decays * master_vec)
    return new_master, new_mean, new_var


def gradients(x, dy, pos_loc, attn_gain, w_query, w_key, w_value, w_out, mlp_gain, w_gate, w_up, w_down):
    wq, wk, wv, wo = w_query.transpose(1, 0, 2), w_key.reshape(DIM, -1), w_value.reshape(DIM, -1), w_out.reshape(DIM, DIM)
    gain_one, gain_two = attn_gain.astype(F32)[None], mlp_gain.astype(F32)[None]
    cos, sin = rope_tables(pos_loc)
    ids = iter(range(1, NDEV))

    normed_t, q, k, v = qkv_call(x, gain_one, wq, wk, wv, cos, sin)
    ctx, ctx_t = attn_fwd(q, k, v)
    hidden, nm, nm_t = oproj_call(ctx, wo, x, gain_two)

    prev, last, parts, gots, squares = None, [], [], [], []
    tiles = FFN // TILE
    ends = [-(-tiles * s // 3) for s in range(4)]
    for lo, hi, when in zip(ends, ends[1:], ((), PLAN["ffn"], PLAN["ffn"])):
        results = ffn_slice(nm, dy, nm_t, w_gate, w_up, w_down, lo, hi - lo, prev, last, when, parts, next(ids))
        prev, (gate, up, gate_r, up_r, *sums, sq) = results[:3], results[3:]
        gots += sums[2:]
        last, parts = [(gate, gate_r), (up, up_r)], list(zip(sums, range(2)))
        squares.append(sq)
    gated_t, d_gate, d_up = prev
    *g_down, part, got_a, got_b, sq = wgrad(
        gated_t, [(dy, 0, DIM)], DOWN_ROWS, 10, ORDER[2], next(ids), last[:1], *PLAN["wgrad"], parts
    )
    squares.append(sq)
    d_hidden, d_low, g_two, up, *downs, got, sq = dn_call(
        d_gate, d_up, w_gate, w_up, hidden, dy, gain_two, last[1], g_down, part, next(ids)
    )
    gots += [got_a, got_b, got]
    squares.append(sq)
    *g_out, _ = wgrad(ctx_t, [(d_low, 0, DIM)], BLK, 4, SAME, next(ids))
    d_context = mm_nt(d_low, wo).astype(BF)
    parts = [(up, 1)] + [(p, 2) for p in downs]
    d_q, d_k, d_v, out_part, *results, sq = attn_bwd(q, k, v, d_context, cos, sin, g_out, g_down, parts, next(ids))
    gots += results[2:]
    squares.append(sq)
    normed_t, out_slab = lax.optimization_barrier((normed_t, attn_flat(out_part, (0, PER))))
    out_all = lax.all_gather(out_slab, "dp", tiled=True)
    parts = [(p, 2) for p in results[:2]]
    rhs = [(d_q, 0, DIM), (d_k, 0, KV_DIM), (d_v, 0, KV_DIM)]
    *g_qkv, got_a, got_b, _ = wgrad(normed_t, rhs, BLK, 4, SAME, next(ids), parts=parts)
    more = [got_a, got_b]
    g_qkv, out_all = lax.optimization_barrier((g_qkv, out_all))
    gate_a, up_a, gate_b, up_b, gate_c, up_c, *downs = gots + more
    slabs = collect([gate_a, gate_b, gate_c], [up_a, up_b, up_c], downs)
    d_x, _, qkv_part, told = dx_call(
        d_q, d_k, d_v, wq, wk, wv, x, gain_one, d_hidden, sum(squares), g_two, g_qkv, next(ids)
    )
    qkv_all = lax.all_gather(attn_flat(qkv_part, (0, PER), (PER, KV_HEADS), (PER + KV_HEADS, KV_HEADS)), "dp")
    gain_sum = jnp.sum(told[:, : 2 * PER], axis=0).astype(BF)
    gain_mean = gain_sum.astype(F32) / NDEV
    grad_norm = jnp.sqrt(jnp.sum(told[:, 2 * PER :]) + jnp.sum(gain_mean * gain_mean))
    return d_x, grad_norm, gain_sum, qkv_all, out_all, slabs


def flat_block(dev, gain_sum, qkv_all, out_all, slabs):
    qn, kn = BLK * PER, BLK * KV_HEADS
    vn = SUB - PER
    head = jnp.concatenate([jnp.zeros((vn, LANES), BF), gain_sum[:PER]])
    v_at = SUB + NDEV * (qn + kn)
    start = (SHARD // LANES + vn) // SUB * SUB
    split, inside = divmod(start - v_at, kn)

    def first():
        pieces = [(0, None, 0, SUB)]
        pieces += [(1, e, 0, qn) for e in SAME] + [(1, e, qn, kn) for e in SAME]
        pieces += [(1, e, qn + kn, kn) for e in SAME[: (WINDOW - v_at) // kn]]
        return paste([head, qkv_all], pieces)

    def second():
        rear = WINDOW + start - v_at - NDEV * (kn + qn)
        tail = jnp.concatenate([gain_sum[PER:], slabs[: rear - PER]])
        pieces = [(0, split, qn + kn + inside, kn - inside)]
        pieces += [(0, e, qn + kn, kn) for e in SAME[split + 1 :]]
        pieces += [(1, None, 0, NDEV * qn), (2, None, 0, rear)]
        return paste([qkv_all, out_all, tail], pieces)

    away = [d * SHARD - (ATTN_ROWS + SLAB * (s or [0])[0]) * LANES for d, s in enumerate(FLAT_SLABS)]
    rows = [max(0, a) // (SUB * LANES) * SUB for a in away]
    rest = [a - r * LANES for a, r in zip(away, rows)]
    rest[:2] = [vn * LANES, SHARD + (vn - start) * LANES]

    def third():
        return lax.dynamic_slice(slabs, (jnp.asarray(rows, jnp.int32)[dev], 0), (WINDOW, LANES))

    window = lax.switch(jnp.minimum(dev, 2), [first, second, third])
    return lax.dynamic_slice(window.reshape(-1), (jnp.asarray(rest, jnp.int32)[dev],), (SHARD,))


def per_device(x_loc, dy_loc, pos_loc, *args):
    *weights, master_loc, mean_loc, var_loc = args
    dev = lax.axis_index("dp")
    d_x, grad_norm, *sums = gradients(x_loc.reshape(TOK, DIM), dy_loc.reshape(TOK, DIM), pos_loc, *weights)
    grad = flat_block(dev, *sums).astype(F32) / NDEV
    new_master, new_mean, new_var = adamw_apply(grad, grad_norm, master_loc, mean_loc, var_loc, dev * SHARD)

    halo = BLOCK * LANES * NDEV - NPARAM
    edge = lax.ppermute(new_master[:halo], "dp", list(zip(SAME[1:], SAME)))
    shift = BLOCK * LANES - SHARD
    block = lax.dynamic_slice(jnp.concatenate([new_master, edge]), (shift * dev,), (BLOCK * LANES,)).astype(BF)
    flat = lax.all_gather(block.reshape(BLOCK, LANES), "dp", tiled=True)

    new, at = [], 0
    for w in weights:
        rows = w.size // LANES
        if w.shape == (DIM, HEADS, LANES):
            new.append(unflat(flat, at, DIM, HEADS, 256, head_major=True).transpose(1, 0, 2))
        elif w.size >= DIM * DIM:
            per = w.shape[-1] // LANES
            new.append(unflat(flat, at, rows // per, per, {COLS: 192}.get(per, 640 if rows > DIM * PER else 256)).reshape(w.shape))
        else:
            new.append(flat[at : at + rows].reshape(w.shape))
        at += rows
    return (d_x.reshape(x_loc.shape), *new, new_master, new_mean, new_var, grad_norm)


def solution(mesh):
    split, same = P("dp"), P()
    in_specs = (split,) * 3 + (same,) * 9 + (split,) * 3
    out_specs = (split,) + (same,) * 9 + (split,) * 3 + (same,)
    return jax.shard_map(per_device, mesh=mesh, in_specs=in_specs, out_specs=out_specs, check_vma=False)
```

```python
import functools

import jax
import jax.numpy as jnp
import numpy as np
from jax import lax
from jax.experimental import pallas as pl
from jax.experimental.pallas import tpu as pltpu
from jax.sharding import PartitionSpec as P

NORM_EPS = 1e-5
ROPE_BASE = 10000.0
LEARN_RATE = 2e-3
BETA_ONE = 0.9
BETA_TWO = 0.95
ADAM_EPS = 1e-8
WEIGHT_DECAY = 0.1
STEP_COUNT = 100
BF = jnp.bfloat16
F32 = jnp.float32
MESH = pl.DeviceIdType.MESH
LANES = 128
SUB = 16
ROWS = SUB // 2
NAXES = 3
TILE = 256
HALF_LANES = LANES // 2
DIM = 1536
HEADS = 12
KV_HEADS = 2
GROUP = HEADS // KV_HEADS
KV_DIM = KV_HEADS * LANES
QKV_DIM = DIM + 2 * KV_DIM
FFN = 8960
SEQ = 768
TOK = 2 * SEQ
NDEV = 16
HALF = NDEV // 2
BLK = DIM // NDEV
NPARAM = 46795776
SHARD = NPARAM // NDEV
COLS = FFN // LANES
PER = DIM // LANES
ATTN_ROWS = PER * (2 + 2 * DIM) + 2 * KV_HEADS * DIM
SLAB = BLK * COLS
SLOTS = 5
DOWN_ROWS = FFN // NDEV // SLOTS
BLOCK = 22856
WINDOW = 22880
SCALE = LANES**-0.5
LOG2_E = float(np.log2(np.e))
HBM = pl.BlockSpec(memory_space=pl.ANY)

HOLDERS = "1b028a37945dc6fe" + "6745e81d9c0a2fb3" + "23b95c081da7ef46"
SLAB_DEV = [int(c, NDEV) for c in HOLDERS]
ORDER = [[SLAB_DEV[w * NDEV : (w + 1) * NDEV].index(d) for d in range(NDEV)] for w in range(3)]
SAME = list(range(NDEV))

PLAN = {
    "ffn": ("0259bb", "148abb"),
    "wgrad": ("136777",),
    "dn": ("14begg", "26fhij", "48imor", "lmoqrr"),
    "attn_bwd": ("1369bb", "247abb", "258bbb"),
    "dx": ("1245",),
}


def mm(a, b):
    return jnp.dot(a, b, preferred_element_type=F32)


def mm_nt(a, b):
    return lax.dot_general(a, b, (((1,), (1,)), ((), ())), preferred_element_type=F32)


def mm_tn(a, b):
    return lax.dot_general(a, b, (((0,), (0,)), ((), ())), preferred_element_type=F32)


def step(c):
    return int(c, 36)


def once(i):
    return pl.when(i == 0)


def row_mean(x):
    return jnp.mean(x, axis=-1, keepdims=True)


def row_sum(x):
    return jnp.sum(x, axis=-1, keepdims=True)


def inv_rms(x):
    return lax.rsqrt(row_mean(x * x) + NORM_EPS)


def spec(shape, index, first=0):
    return pl.BlockSpec(shape, lambda *g: tuple(0 if c == "." else g["ijk".index(c)] + first for c in index))


def full(shape):
    return pl.BlockSpec(shape, lambda *_: (0,) * len(shape), pipeline_mode=pl.Buffered(1))


def bf(*shapes):
    return [jax.ShapeDtypeStruct(s, BF) for s in shapes]


def f32(*shapes):
    return [jax.ShapeDtypeStruct(s, F32) for s in shapes]


def dma(*shape):
    return pltpu.SemaphoreType.DMA(shape)


def pcall(kernel, *, grid, in_specs, out_specs, out_shape, name, scratch=(), carry=(), cid=None):
    carry = list(carry or ())
    head, skip = len(in_specs), len(carry)

    def body(*refs):
        kernel(*refs[:head], *refs[head + skip :])

    remote = {} if cid is None else dict(collective_id=cid, has_side_effects=True)
    call = pl.pallas_call(
        body,
        grid=grid,
        in_specs=list(in_specs) + [HBM] * skip,
        out_specs=out_specs,
        scratch_shapes=list(scratch),
        out_shape=out_shape,
        input_output_aliases={head + j: j for j in range(skip)},
        compiler_params=pltpu.CompilerParams(vmem_limit_bytes=63 << 20, **remote),
        cost_estimate=pl.CostEstimate(flops=NPARAM * TILE, bytes_accessed=NPARAM, transcendentals=0),
        name=name,
    )
    return lambda *args: call(*args, *carry)


def flat_slabs(d):
    block = SHARD / LANES
    lo = max(0, int((d * block - ATTN_ROWS) // SLAB))
    hi = int(-(-((d + 1) * block - ATTN_ROWS) // SLAB))
    return list(range(lo, min(hi, 3 * NDEV)))


FLAT_SLABS = [flat_slabs(d) for d in range(NDEV)]


def pick(table, me):
    value = jnp.int32(table[0])
    for d in SAME[1:]:
        value = jnp.where(me == d, jnp.int32(table[d]), value)
    return value


AXES = [[(g + s) % NAXES for s in range(NAXES)] for g in range(NAXES)]
LOCAL, FINAL, NSEM = range(10, 13)


def remote_copy(src, dst, send, recv, device):
    return pltpu.make_async_remote_copy(src, dst, send, recv, device_id=(device,), device_id_type=MESH)


class Scatter:
    def __init__(self, a, out, bufs, n, width, sq, row0=0):
        self.a, self.out, self.n, self.sq, self.rows = a, out, n, sq, pl.ds(row0, n)
        self.keep, *self.got, self.sems = bufs
        chunks = width // LANES
        ends = [chunks * g // NAXES * LANES for g in range(4)]
        self.cols = [pl.ds(lo, hi - lo) for lo, hi in zip(ends, ends[1:])]
        self.me = lax.axis_index("dp")
        self.chip = self.me // 2
        self.bits = [lax.rem(self.chip // (1 << b), 2) for b in range(NAXES)]

    @staticmethod
    def scratch(n, width):
        return [pltpu.VMEM((k, n, width), BF) for k in (HALF, HALF, 4, 2, 1)] + [dma(2, NSEM)]

    def remote(self, src, dst, k, device):
        return remote_copy(src, dst, self.sems.at[0, k], self.sems.at[1, k], device)

    def whole(self, stage, g):
        ref = self.got[stage + 1].at[:, :, self.cols[g]]
        return self.remote(ref, ref, 1 + NAXES * stage + g, self.me ^ 1)

    def loads(self):
        for k, dst in enumerate((self.keep, self.got[0])):
            yield pltpu.make_async_copy(self.a[k].at[:, self.rows, :], dst, self.sems.at[k, LOCAL])

    def start(self):
        for copy in self.loads():
            copy.start()

    def block(self, g, stage, t, send):
        axes = AXES[g]
        own = self.bits[axes[stage]]
        j = (1 - own if send else own) * (1 << axes[stage])
        for s in axes[:stage]:
            j += self.bits[s] * (1 << s)
        for r, s in enumerate(axes[stage + 1 :]):
            j += ((t >> r) & 1) * (1 << s)
        return j

    def push(self, stage):
        for g, axes in enumerate(AXES):
            for t in range(4 >> stage):
                src = self.keep.at[self.block(g, stage, t, True), :, self.cols[g]]
                dst = self.got[stage + 1].at[t, :, self.cols[g]]
                self.remote(src, dst, 1 + NAXES * stage + g, self.me ^ (2 << axes[stage])).start()

    def sum_rows(self, j, src, cols):
        def body(r, _):
            sl = pl.ds(pl.multiple_of(r * SUB, SUB), SUB)
            self.keep[j, sl, cols] = self.keep[j, sl, cols] + src[sl, cols]
            return 0

        lax.fori_loop(0, self.n // SUB, body, 0)

    def first(self):
        for copy in self.loads():
            copy.wait()

        def body(j, _):
            self.sum_rows(j, self.got[0].at[j], slice(None))
            return 0

        lax.fori_loop(0, HALF, body, 0)
        self.push(0)

    def merge(self, stage):
        for g in range(NAXES):
            self.whole(stage, g).wait_recv()
            for t in range(4 >> stage):
                self.sum_rows(self.block(g, stage, t, False), self.got[stage + 1].at[t], self.cols[g])
        if stage < 2:
            self.push(stage + 1)

    def hand_over(self):
        return pltpu.make_async_copy(self.keep.at[self.chip], self.out, self.sems.at[0, FINAL])

    def last(self):
        self.merge(2)
        self.hand_over().start()

        def body(r, _):
            g = self.keep[self.chip, pl.ds(pl.multiple_of(r * SUB, SUB), SUB), :].astype(F32) * (1.0 / NDEV)
            g = g * g
            total = g[: ROWS] + g[ROWS :]
            for c in range(0, total.shape[1], LANES):
                self.sq[:] += total[:, c : c + LANES]
            return 0

        lax.fori_loop(0, self.n // SUB, body, 0)

    def finish(self):
        self.hand_over().wait()
        for stage in range(NAXES):
            for g in range(NAXES):
                self.whole(stage, g).wait_send()

    def run(self, i, at, final=NPARAM):
        stages = (self.start, self.first, *(functools.partial(self.merge, s) for s in range(2)), self.last, self.finish)
        for c, todo in zip(at, stages):
            k = min(step(c), final)
            if isinstance(i, int):
                if i == k:
                    todo()
            else:
                pl.when(i == k)(todo)

    def hand_on(self, sem):
        for k in (1, 2, 4, 8):
            pl.semaphore_signal(sem, inc=1, device_id=(self.me ^ k,), device_id_type=MESH)


class Push:
    def __init__(self, src, got, sems, weight):
        self.src, self.got, self.sems, self.weight = src, got, sems, weight
        self.me = lax.axis_index("dp")

    def each(self):
        held = [self.weight * NDEV + b for b in ORDER[self.weight]]
        for k in range(2):
            own = [([d for d in SAME if h in FLAT_SLABS[d]][k:] or [-1])[0] for h in held]
            slot = [FLAT_SLABS[d].index(h) if d >= 0 else 0 for d, h in zip(own, held)]
            to, slot = pick(own, self.me), pick(slot, self.me)
            dst, recv = self.got.at[slot], self.sems.at[1, slot]
            there = remote_copy(self.src, dst, self.sems.at[0, k], recv, jnp.maximum(to, 0))
            yield to, pltpu.make_async_copy(self.src, dst, recv), there

    def start(self):
        for to, here, there in self.each():
            pl.when(to == self.me)(here.start)
            pl.when((to >= 0) & (to != self.me))(there.start)

    def finish(self):
        for to, _, there in self.each():
            pl.when((to >= 0) & (to != self.me))(there.wait_send)
        for j in range(SLOTS):
            gets = [len(s) > j and s[j] // NDEV == self.weight for s in FLAT_SLABS]
            pl.when(pick(gets, self.me) == 1)(pltpu.make_async_copy(self.src, self.got.at[j], self.sems.at[1, j]).wait)


def push_all(refs, weights, start):
    n = len(weights)
    for j, w in enumerate(weights):
        job = Push(*refs[j::n], w)
        (job.start if start else job.finish)()


SLOT_SEMS = dma(2, SLOTS)


def push_shapes(parts):
    return bf(*((SLOTS, *p.shape) for p, _ in parts))


def push_sems(parts):
    return [SLOT_SEMS] * len(parts)


def greet():
    me = lax.axis_index("dp")
    for k in SAME[1:]:
        pl.semaphore_signal(pltpu.get_barrier_semaphore(), inc=1, device_id=(me ^ k,), device_id_type=MESH)


def met():
    pl.semaphore_wait(pltpu.get_barrier_semaphore(), NDEV - 1)


SQ_SPEC = full((ROWS, LANES))
SQ = f32((ROWS, LANES))


def blocks(pairs):
    return [g.reshape(HALF, -1, g.shape[-1]) for pair in pairs for g in pair]


def row_block(order, p, core):
    j, mine = 2 * (p % HALF), p // HALF
    return jnp.where(core == mine, order[j + 1], order[j])


def head_pair(w_ref, h):
    return jnp.concatenate([w_ref[h], w_ref[h + 1]], axis=1)


def qkv_kernel(x_ref, g_ref, wq_ref, wk_ref, wv_ref, c_ref, s_ref, nt_ref, q_ref, k_ref, v_ref):
    x = x_ref[:].astype(F32)
    inv = inv_rms(x)
    n = (x * inv * g_ref[:]).astype(BF)
    nt_ref[:] = n.T
    c, s = c_ref[:], s_ref[:]

    def rope(out, t, h):
        for j in range(2):
            u = t[:, j * LANES : (j + 1) * LANES]
            cols = slice((h + j) * LANES, (h + j + 1) * LANES)
            out[:, cols] = (u * c + pltpu.roll(u, HALF_LANES, 1) * s).astype(BF)

    for h in range(0, HEADS, 2):
        rope(q_ref, mm(n, head_pair(wq_ref, h)), h)
    rope(k_ref, mm(n, wk_ref[:]), 0)
    v_ref[:] = mm(n, wv_ref[:]).astype(BF)


def qkv_call(x, gain, wq, wk, wv, cos, sin, tile=TILE):
    r = lambda w: spec((tile, w), "i.")
    return pcall(
        qkv_kernel,
        grid=(TOK // tile,),
        in_specs=[r(DIM), full(gain.shape), full(wq.shape), full(wk.shape), full(wv.shape), r(LANES), r(LANES)],
        out_specs=[spec((DIM, tile), ".i"), r(DIM), r(KV_DIM), r(KV_DIM)],
        out_shape=bf((DIM, TOK), (TOK, DIM), (TOK, KV_DIM), (TOK, KV_DIM)),
        name="qkv",
    )(x, gain, wq, wk, wv, cos, sin)


def probs(q, k, i, bq):
    s = mm_nt(q, k[: (i + 1) * bq])
    r = lax.broadcasted_iota(jnp.int32, (bq, bq), 0)
    c = lax.broadcasted_iota(jnp.int32, (bq, bq), 1)
    d = jnp.where(r >= c, s[:, i * bq :], -1e30)
    s = jnp.concatenate([s[:, : i * bq], d], axis=1) if i else d
    e = jnp.exp2((s - jnp.max(s, axis=-1, keepdims=True)) * (SCALE * LOG2_E))
    return e * (1.0 / row_sum(e))


def head_cols(h):
    return slice(h * LANES, (h + 1) * LANES)


def attn_fwd_kernel(q_ref, k_ref, v_ref, o_ref, ot_ref, *, bq):
    k, v = k_ref[:], v_ref[:]
    for i in range(SEQ // bq):
        r = slice(i * bq, (i + 1) * bq)
        for c in map(head_cols, range(GROUP)):
            p = probs(q_ref[r, c], k, i, bq).astype(BF)
            o = mm(p, v[: (i + 1) * bq]).astype(BF)
            o_ref[r, c] = o
            ot_ref[c, r] = o.T


def attn_fwd(q, k, v, bq=384):
    hq, hk = spec((SEQ, GROUP * LANES), "ij"), spec((SEQ, LANES), "ij")
    return pcall(
        functools.partial(attn_fwd_kernel, bq=bq),
        grid=(TOK // SEQ, KV_HEADS),
        in_specs=[hq, hk, hk],
        out_specs=[hq, spec((GROUP * LANES, SEQ), "ji")],
        out_shape=bf((TOK, DIM), (DIM, TOK)),
        name="attn_fwd",
    )(q, k, v)


def attn_bwd_kernel(q_ref, k_ref, v_ref, do_ref, c_ref, s_ref, out_k, out_r, down_k, down_r, *refs, weights, bq, nh):
    nw = len(weights)
    ins, (dq_ref, dk_ref, dv_ref, out_out, down_a, down_b), refs = refs[:nw], refs[nw:][:6], refs[nw + 6 :]
    gots, (sq, dka, dva), sems, refs = refs[:nw], refs[nw:][:3], refs[nw + 3 :][:nw], refs[2 * nw + 3 :]
    pushes = (*ins, *gots, *sems)
    b, kv, group = (pl.program_id(j) for j in range(NAXES))
    steps = GROUP // nh
    i = (b * KV_HEADS + kv) * steps + group
    n = DOWN_ROWS

    @once(i)
    def _():
        sq[:] = jnp.zeros_like(sq)
        greet()

    @pl.when(i == step("1"))
    def _():
        met()
        push_all(pushes, weights, True)

    down, plan = (down_k, down_r), PLAN["attn_bwd"]
    Scatter(down, down_a, refs[:6], n, DIM, sq, 3 * n).run(i, plan[0])
    Scatter(down, down_b, refs[6:12], n, DIM, sq, 4 * n).run(i, plan[1])
    Scatter((out_k, out_r), out_out, refs[12:], BLK, DIM, sq).run(i, plan[2])
    pl.when(i == step(plan[0][-1]))(lambda: push_all(pushes, weights, False))
    k, v = k_ref[:], v_ref[:]

    @once(group)
    def _():
        dka[:] = jnp.zeros_like(dka)
        dva[:] = jnp.zeros_like(dva)

    def back(t, c, s):
        return (t * c - pltpu.roll(t, HALF_LANES, 1) * s).astype(BF)

    for i in range(SEQ // bq):
        r, w = slice(i * bq, (i + 1) * bq), (i + 1) * bq
        sides = [[], [], [], []]
        for c in map(head_cols, range(nh)):
            q, do = q_ref[r, c], do_ref[r, c]
            p = probs(q, k, i, bq)
            dp = mm_nt(do, v[:w])
            ds = (p * (dp - row_sum(dp * p)) * SCALE).astype(BF)
            dq_ref[r, c] = back(mm(ds, k[:w]), c_ref[r, :], s_ref[r, :])
            for side, value in zip(sides, (ds, q, p.astype(BF), do)):
                side.append(value)
        ds, q, p, do = (jnp.concatenate(side, axis=0) for side in sides)
        dka[:w, :] += mm_tn(ds, q)
        dva[:w, :] += mm_tn(p, do)

    @pl.when(group == steps - 1)
    def _():
        dk_ref[:] = back(dka[:], c_ref[:], s_ref[:])
        dv_ref[:] = dva[:].astype(BF)


def attn_bwd(q, k, v, do, cos, sin, g_out, g_down, parts, cid, bq=384, nh=2):
    steps = GROUP // nh
    hq = pl.BlockSpec((SEQ, nh * LANES), lambda b, kv, g: (b, kv * steps + g))
    hk = spec((SEQ, LANES), "ij")
    tb = spec((SEQ, LANES), "i.")
    down = (DOWN_ROWS, DIM)
    return pcall(
        functools.partial(attn_bwd_kernel, weights=[w for _, w in parts], bq=bq, nh=nh),
        grid=(TOK // SEQ, KV_HEADS, steps),
        in_specs=[hq, hk, hk, hq, tb, tb] + [HBM] * (4 + len(parts)),
        out_specs=[hq, hk, hk] + [HBM] * (3 + len(parts)) + [SQ_SPEC],
        out_shape=bf((TOK, DIM), k.shape, v.shape, (BLK, DIM), down, down) + push_shapes(parts) + SQ,
        scratch=[pltpu.VMEM((SEQ, LANES), F32)] * 2
        + push_sems(parts)
        + Scatter.scratch(*down) * 2
        + Scatter.scratch(BLK, DIM),
        name="attn_bwd",
        cid=cid,
    )(q, k, v, do, cos, sin, *blocks([g_out, g_down]), *[p for p, _ in parts])


def oproj_kernel(c_ref, wo_ref, x_ref, g_ref, h_ref, n_ref, nt_ref):
    h = (x_ref[:].astype(F32) + mm(c_ref[:], wo_ref[:])).astype(BF)
    h_ref[:] = h
    hw = h.astype(F32)
    inv = inv_rms(hw)
    n = (hw * inv * g_ref[:]).astype(BF)
    n_ref[:] = n
    nt_ref[:] = n.T


def oproj_call(ctx, wo, x, gain, tile=TILE):
    r = spec((tile, DIM), "i.")
    return pcall(
        oproj_kernel,
        grid=(TOK // tile,),
        in_specs=[r, full(wo.shape), r, full(gain.shape)],
        out_specs=[r, r, spec((DIM, tile), ".i")],
        out_shape=bf((TOK, DIM), (TOK, DIM), (DIM, TOK)),
        name="oproj",
    )(ctx, wo, x, gain)


def ffn_kernel(nm_h, dy_h, nt_h, wg_ref, wu_ref, wd_ref, *refs, units, at, weights, count, rc):
    nu, nw = len(units), len(weights)
    ins, refs = refs[: 2 * nu + nw], refs[2 * nu + nw :]
    (gt_ref, dg_ref, du_ref, gg_ref, gu_ref, rg_h, ru_h), refs = refs[:7], refs[7:]
    outs, (sq, nm, dy, na, nb, out, sem, core_sem), refs = refs[: nu + nw], refs[nu + nw :][:8], refs[nu + nw + 8 :]
    pushes = (*ins[2 * nu :], *outs[nu:], *refs[:nw])
    i = pl.program_id(0)
    me = lax.axis_index("dp")
    half, tile = out.shape[-2:]
    loads = [(nm_h, nm), (dy_h, dy), (nt_h, na), (nt_h, nb)]

    @once(i)
    def _():
        sq[:] = jnp.zeros_like(sq)
        for j, (src, dst) in enumerate(loads):
            if src is not nt_h:
                pltpu.make_async_copy(src, dst, sem.at[j]).start()
                continue
            for p in range(NDEV):
                b = row_block(ORDER[j - 2], p, lax.rem(me, 2))
                rows = src.at[pl.ds(pl.multiple_of(b * BLK, BLK), BLK)]
                pltpu.make_async_copy(rows, dst.at[pl.ds(p * BLK, BLK)], sem.at[j]).start()
        greet()

    jobs = [
        Scatter(ins[2 * u :][:2], outs[u], refs[nw + 6 * u :][:6], *unit, sq) for u, unit in enumerate(units)
    ]

    @once(i)
    def _():
        for j, (src, dst) in enumerate(loads):
            pltpu.make_async_copy(src, dst, sem.at[j]).wait()

    slot = lax.rem(i, 2)

    def across(w, dst, t):
        cols = dst.at[:, pl.ds(pl.multiple_of(t * tile, tile), tile)]
        slot = lax.rem(t, 2)
        return remote_copy(out.at[slot, w], cols, core_sem.at[slot, w], core_sem.at[2, w], me ^ 1)

    @pl.when(i >= 2)
    def _():
        for w, dst in enumerate((rg_h, ru_h)):
            across(w, dst, i - 2).wait_send()

    for r in range(0, TOK, rc):
        sl = pl.ds(r, rc)
        gate = mm(nm[sl, :], wg_ref[:])
        up = mm(nm[sl, :], wu_ref[:])
        dga = mm_nt(dy[sl, :], wd_ref[:])
        sig = 1.0 / (1.0 + jnp.exp(-gate))
        act = gate * sig
        gt_ref[:, sl] = (act * up).astype(BF).T
        du_ref[sl, :] = (dga * act).astype(BF)
        dg_ref[sl, :] = (dga * up * sig * (1.0 + gate * (1.0 - sig))).astype(BF)

    @once(i)
    def _():
        met()
        push_all(pushes, weights, True)

    for job, when in zip(jobs, at):
        job.run(i, when, count - 1)
    if nw:
        pl.when(i == count - 1)(lambda: push_all(pushes, weights, False))
    for w, (src, rhs, keep) in enumerate(((na, dg_ref, gg_ref), (nb, du_ref, gu_ref))):
        out[slot, w] = mm(src[:half, :], rhs[:]).astype(BF)
        keep[:] = mm(src[half:, :], rhs[:]).astype(BF)
    for w, dst in enumerate((rg_h, ru_h)):
        across(w, dst, i).start()

        @pl.when(i == count - 1)
        def _(w=w, dst=dst):
            across(w, dst, i - 1).wait_send()
            across(w, dst, i).wait_send()
            remote_copy(dst, dst, core_sem.at[0, w], core_sem.at[2, w], me ^ 1).wait_recv()


def ffn_slice(nm, dy, nt, wg, wu, wd, first, count, prev, arrays, at, parts, cid, tile=TILE, rc=TILE):
    width, half = count * tile, DIM // 2
    units = [(BLK, g.shape[-1]) for g, _ in arrays]
    nmore = len(units) + len(parts)
    col, row, grad = spec((DIM, tile), ".i", first), spec((tile, DIM), "i.", first), spec((half, tile), ".i")
    outs = bf((FFN, TOK), (TOK, FFN), (TOK, FFN), *[(half, width)] * 4, *units)
    return pcall(
        functools.partial(ffn_kernel, units=units, at=at, weights=[w for _, w in parts], count=count, rc=rc),
        grid=(count,),
        in_specs=[HBM] * 3 + [col, col, row] + [HBM] * (nmore + len(units)),
        out_specs=[row, col, col, grad, grad] + [HBM] * (2 + nmore) + [SQ_SPEC],
        out_shape=outs + push_shapes(parts) + SQ,
        scratch=[pltpu.VMEM((TOK, DIM), BF)] * 4
        + [pltpu.VMEM((2, 2, half, tile), BF), dma(4), dma(3, 2)]
        + push_sems(parts)
        + [t for u in units for t in Scatter.scratch(*u)],
        name="ffn",
        carry=prev,
        cid=cid,
    )(nm, dy, nt, wg, wu, wd, *blocks(arrays), *[p for p, _ in parts])


def wgrad_kernel(lhs_h, *refs, cols, nr, per, blk, order, units, at, weights):
    nrhs, nu, nw = len(cols), len(units), len(weights)
    nm = nu + nw
    rhs_h, ins, (keep_h, other_h, *refs) = refs[:nrhs], refs[nrhs:][: nm + nu], refs[nrhs + nm + nu :]
    outs, (sq, *refs) = refs[:nm], refs[nm:]
    me = lax.axis_index("dp")
    rhs, (lhs, out, sem_l, sem_r, sem_o), refs = refs[:nrhs], refs[nrhs:][:5], refs[nrhs + 5 :]
    pushes = (*ins[2 * nu :], *outs[nu:], *refs[:nw])
    size = per * nr
    steps = NDEV * blk // size
    ring = lhs.shape[0]

    def fetch(t):
        for j in range(per):
            p, r = divmod((t * per + j) * nr, blk)
            src = lhs_h.at[pl.ds(pl.multiple_of(row_block(order, p, lax.rem(me, 2)) * blk + r, SUB), nr)]
            pltpu.make_async_copy(src, lhs.at[t % ring, pl.ds(j * nr, nr)], sem_l.at[t % ring]).start()

    def rhs_copy(j):
        c, w = cols[j]
        return pltpu.make_async_copy(rhs_h[j].at[:, pl.ds(c, w)], rhs[j], sem_r.at[j])

    def remote(src, dst, slot):
        return remote_copy(src, dst, sem_o.at[slot], sem_o.at[2], me ^ 1)

    def out_copy(t, wait):
        src, slot, half = out.at[t % 2], t % 2, steps // 2
        if t < half:
            copy = remote(src, other_h.at[pl.ds(t * size, size)], slot)
            (copy.wait_send if wait else copy.start)()
        else:
            copy = pltpu.make_async_copy(src, keep_h.at[pl.ds((t - half) * size, size)], sem_o.at[slot])
            (copy.wait if wait else copy.start)()

    fetch(0)
    for j in range(nrhs):
        rhs_copy(j).start()
    fetch(1)
    sq[:] = jnp.zeros_like(sq)
    greet()
    jobs = [Scatter(ins[2 * u :][:2], outs[u], refs[nw + 6 * u :][:6], *unit, sq) for u, unit in enumerate(units)]
    for t in range(steps):
        if t + 2 < steps:
            fetch(t + 2)
        pltpu.make_async_copy(lhs_h.at[pl.ds(0, size)], lhs.at[t % ring], sem_l.at[t % ring]).wait()
        if t >= 2:
            out_copy(t - 2, True)
        c = 0
        for j in range(nrhs):
            if t == 0:
                rhs_copy(j).wait()
            o = mm(lhs[t % ring], rhs[j][:]).astype(BF)
            out[t % 2, :, c : c + o.shape[1]] = o
            c += o.shape[1]
        if t == 0:
            met()
            push_all(pushes, weights, True)
        out_copy(t, False)
        for job in jobs:
            job.run(t, at)
    for t in range(steps - 2, steps):
        out_copy(t, True)
    remote(other_h, other_h, 0).wait_recv()
    push_all(pushes, weights, False)


def wgrad(lhs_t, rhs, nr, per, order, cid, arrays=(), at="", parts=()):
    rows, width = lhs_t.shape[0], sum(w for _, _, w in rhs)
    units = [(BLK, g.shape[-1]) for g, _ in arrays]
    nmore = len(units) + len(parts)
    return pcall(
        functools.partial(
            wgrad_kernel,
            cols=[r[1:] for r in rhs],
            nr=nr,
            per=per,
            blk=rows // NDEV,
            order=order,
            units=units,
            at=at,
            weights=[w for _, w in parts],
        ),
        grid=(1,),
        in_specs=[HBM] * (1 + len(rhs) + nmore + len(units)),
        out_specs=[HBM] * (2 + nmore) + [SQ_SPEC],
        out_shape=bf(*[(rows // 2, width)] * 2, *units) + push_shapes(parts) + SQ,
        scratch=[pltpu.VMEM((TOK, w), BF) for _, _, w in rhs]
        + [pltpu.VMEM((3, per * nr, TOK), BF), pltpu.VMEM((2, per * nr, width), BF), dma(3), dma(len(rhs)), dma(3)]
        + push_sems(parts)
        + [t for u in units for t in Scatter.scratch(*u)],
        name="wgrad",
        cid=cid,
    )(lhs_t, *[r[0] for r in rhs], *blocks(arrays), *[p for p, _ in parts])


def norm_back(d, x, g_ref, gg_ref):
    inv = inv_rms(x)
    hat = x * inv
    gg_ref[:] += jnp.sum(d * hat, axis=0, keepdims=True)
    dg = d * g_ref[:]
    return inv * (dg - hat * row_mean(dg * hat))


def dn_kernel(dg_ref, du_ref, wg_ref, wu_ref, h_ref, dy_ref, g_ref, up_k, up_r, down_k, down_r, part_h, dh_ref, dl_ref, gg_ref, *refs, up):
    up_out, down_a, down_b, down_c, got, got_up, got_a, sq, acc, ready, psem, usem, asem, *refs = refs
    push, push_up, push_a = Push(part_h, got, psem, 0), Push(up_out, got_up, usem, 1), Push(down_a, got_a, asem, 2)
    t, k = pl.program_id(0), pl.program_id(1)
    i = t * pl.num_programs(1) + k
    n = DOWN_ROWS

    @once(i)
    def _():
        gg_ref[:] = jnp.zeros_like(gg_ref)
        sq[:] = jnp.zeros_like(sq)
        greet()

    @pl.when(i == step("1"))
    def _():
        met()
        push.start()

    plan = PLAN["dn"]
    up_h, down_h = (up_k, up_r), (down_k, down_r)
    one = Scatter(down_h, down_a, refs[6:12], n, DIM, sq)
    three = Scatter(down_h, down_c, refs[6:11] + refs[18:], n, DIM, sq, 2 * n)
    Scatter(up_h, up_out, refs[:6], *up, sq).run(i, plan[0])
    one.run(i, plan[1])
    Scatter(down_h, down_b, refs[12:18], n, DIM, sq, n).run(i, plan[2])
    pl.when(i == step(plan[1][-1]))(lambda: one.hand_on(ready))
    pl.when(i == step(plan[3][0]))(lambda: pl.semaphore_wait(ready, 4))
    three.run(i, plan[3])
    pl.when(i == step(plan[0][-1]) + 1)(push_up.start)
    pl.when(i == step(plan[1][-1]) + 1)(push_a.start)

    @pl.when(i == step("r"))
    def _():
        for job in (push, push_up, push_a):
            job.finish()


    @once(k)
    def _():
        acc[:] = jnp.zeros_like(acc)

    acc[:] += mm_nt(dg_ref[:], wg_ref[:]) + mm_nt(du_ref[:], wu_ref[:])

    @pl.when(k == pl.num_programs(1) - 1)
    def _():
        def body(r, _):
            sl = pl.ds(pl.multiple_of(r * LANES, LANES), LANES)
            o = norm_back(acc[sl, :], h_ref[sl, :].astype(F32), g_ref, gg_ref) + dy_ref[sl, :].astype(F32)
            dh_ref[sl, :] = o
            dl_ref[sl, :] = o.astype(BF)
            return 0

        lax.fori_loop(0, acc.shape[0] // LANES, body, 0)


def dn_call(dg, du, wg, wu, h, dy, gain, g_up, g_down, part, cid, tt=384, tk=1280):
    up, down = (BLK, g_up[0].shape[-1]), (DOWN_ROWS, DIM)
    act, wgt, row = spec((tt, tk), "ij"), spec((DIM, tk), ".j"), spec((tt, DIM), "i.")
    gained = spec(gain.shape, "..")
    return pcall(
        functools.partial(dn_kernel, up=up),
        grid=(TOK // tt, FFN // tk),
        in_specs=[act, act, wgt, wgt, row, row, full(gain.shape)] + [HBM] * 5,
        out_specs=[row, row, gained] + [HBM] * 7 + [SQ_SPEC],
        out_shape=f32((TOK, DIM)) + bf((TOK, DIM)) + f32(gain.shape) + bf(up, *[down] * 3, *[(SLOTS, *t) for t in (part.shape, up, down)]) + SQ,
        scratch=[pltpu.VMEM((tt, DIM), F32), pltpu.SemaphoreType.REGULAR]
        + [SLOT_SEMS] * 3
        + Scatter.scratch(*up)
        + Scatter.scratch(*down) * 2
        + Scatter.scratch(*down)[-1:],
        name="dn",
        cid=cid,
    )(dg, du, wg, wu, h, dy, gain, *blocks([g_up, g_down]), part)


def dx_kernel(
    dq_ref, dk_ref, dv_ref, wq_ref, wk_ref, wv_ref, x_ref, g_ref, dh_ref, sq_ref, g_two_ref, qkv_k, qkv_r,
    dx_ref, gg_ref, qkv_out, told_ref, sq, mine, told, tell, *refs,
):
    i = pl.program_id(0)

    @once(i)
    def _():
        gg_ref[:] = jnp.zeros_like(gg_ref)
        sq[:] = sq_ref[:]
        greet()

    pl.when(i == step("1"))(met)
    scatter = Scatter((qkv_k, qkv_r), qkv_out, refs, BLK, QKV_DIM, sq)
    scatter.run(i, *PLAN["dx"])
    d = mm_nt(dk_ref[:], wk_ref[:]) + mm_nt(dv_ref[:], wv_ref[:])
    for h in range(0, HEADS, 2):
        d += mm_nt(dq_ref[:, h * LANES : (h + 2) * LANES], head_pair(wq_ref, h))
    dx_ref[:] = (norm_back(d, x_ref[:].astype(F32), g_ref, gg_ref) + dh_ref[:]).astype(BF)

    @pl.when(i == pl.num_programs(0) - 1)
    def _():
        scatter.last()
        for row, ref in enumerate((gg_ref, g_two_ref)):
            for c in range(PER):
                mine[pl.ds(row * PER + c, 1), :] = ref[:, head_cols(c)].astype(BF).astype(F32)
        mine[2 * PER :, :] = sq[:]
        me = lax.axis_index("dp")
        copies = []
        for k in SAME[1:]:
            copies.append(remote_copy(mine, told.at[me], tell.at[0, k], tell.at[1, k], me ^ k))
            copies[-1].start()
        told[me] = mine[:]
        for copy in copies:
            copy.wait()
        told_ref[:] = told[:]
        scatter.finish()


def dx_call(dq, dk, dv, wq, wk, wv, x, gain, dh, squares, g_two, g_qkv, cid, tile=TILE):
    r = lambda w: spec((tile, w), "i.")
    told = (2 * PER + squares.shape[0], LANES)
    return pcall(
        dx_kernel,
        grid=(TOK // tile,),
        in_specs=[r(DIM), r(KV_DIM), r(KV_DIM), full(wq.shape), full(wk.shape), full(wv.shape), r(DIM), full(gain.shape)]
        + [r(DIM), SQ_SPEC, full(gain.shape), HBM, HBM],
        out_specs=[r(DIM), spec(gain.shape, ".."), HBM, full((NDEV, *told))],
        out_shape=bf((TOK, DIM)) + f32(gain.shape) + bf((BLK, QKV_DIM)) + f32((NDEV, *told)),
        scratch=[pltpu.VMEM(squares.shape, F32), pltpu.VMEM(told, F32), pltpu.VMEM((NDEV, *told), F32), dma(2, NDEV)] + Scatter.scratch(BLK, QKV_DIM),
        name="dx",
        cid=cid,
    )(dq, dk, dv, wq, wk, wv, x, gain, dh, squares, g_two, *blocks([g_qkv]))


def to_lane_rows(wide, base, per, part, col, rows):
    for j in range(part.shape[1] // LANES):
        piece = part[:, j * LANES : (j + 1) * LANES].astype(F32)
        wide[pl.ds(base + col + j, rows, stride=per), :] = piece


def attn_flat_kernel(x_ref, o_ref, wide, *, segs):
    base = 0
    for col, per in segs:
        to_lane_rows(wide, base, per, x_ref[:, col * LANES : (col + per) * LANES], 0, BLK)
        base += BLK * per
    o_ref[:] = wide[:].astype(BF)


def attn_flat(x, *segs):
    rows = x.size // LANES
    return pcall(
        functools.partial(attn_flat_kernel, segs=segs),
        grid=(1,),
        in_specs=[full(x.shape)],
        out_specs=full((rows, LANES)),
        out_shape=bf((rows, LANES))[0],
        scratch=[pltpu.VMEM((rows, LANES), F32)],
        name="attn_flat",
    )(x)


def collect_kernel(*refs, ng, nd):
    gates, ups, downs = refs[:ng], refs[ng : 2 * ng], refs[2 * ng : 2 * ng + nd]
    o_h, tall, flat, wide, out, sem = refs[2 * ng + nd :]
    me = lax.axis_index("dp")
    kinds = [[s[k] // NDEV if k < len(s) else -1 for s in FLAT_SLABS] for k in range(SLOTS)]

    def copies(k, parts, dst, axis):
        at = 0
        for p in parts:
            n = p.shape[axis]
            to = dst.at[:, pl.ds(at, n)] if axis == 2 else dst.at[pl.ds(at, n)]
            yield pltpu.make_async_copy(p.at[k], to, sem.at[0])
            at += n

    for k in range(SLOTS):
        kind = pick(kinds[k], me)
        for w, parts in enumerate((gates, ups, downs)):

            @pl.when(kind == w)
            def _(k=k, w=w, parts=parts):
                todo = list(copies(k, parts, *((tall, 1) if w == 2 else (flat, 2))))
                for c in todo:
                    c.start()
                for c in todo:
                    c.wait()

        def store(k=k):
            return pltpu.make_async_copy(out, o_h.at[pl.ds(k * SLAB, SLAB)], sem.at[1])

        @pl.when(kind == 2)
        def _():
            to_lane_rows(wide, 0, PER, tall, 0, tall.shape[0])

        @pl.when((kind == 0) | (kind == 1))
        def _():
            to_lane_rows(wide, 0, COLS, flat, 0, BLK)

        if k:
            store(k - 1).wait()
        out[:] = wide[:].astype(BF)
        store().start()
    store().wait()


def collect(gates, ups, downs):
    parts = [*gates, *ups, *downs]
    return pcall(
        functools.partial(collect_kernel, ng=len(gates), nd=len(downs)),
        grid=(1,),
        in_specs=[HBM] * len(parts),
        out_specs=HBM,
        out_shape=bf((SLOTS * SLAB, LANES))[0],
        scratch=[
            pltpu.VMEM((FFN // NDEV, DIM), BF),
            pltpu.VMEM((BLK, FFN), BF),
            pltpu.VMEM((SLAB, LANES), F32),
            pltpu.VMEM((SLAB, LANES), BF),
            dma(2),
        ],
        name="collect",
    )(*parts)


def paste_kernel(*refs, pieces):
    srcs, (o_ref, sem) = refs[:-2], refs[-2:]
    todo = []
    for s, lead, row, n, dst in pieces:
        src = srcs[s] if lead is None else srcs[s].at[lead]
        todo.append(pltpu.make_async_copy(src.at[pl.ds(row, n)], o_ref.at[pl.ds(dst, n)], sem.at[len(todo)]))
    for c in todo:
        c.start()
    for c in todo:
        c.wait()


def paste(srcs, pieces):
    placed, at = [], 0
    for p in pieces:
        placed.append((*p, at))
        at += p[-1]
    return pcall(
        functools.partial(paste_kernel, pieces=placed),
        grid=(1,),
        in_specs=[HBM] * len(srcs),
        out_specs=full((WINDOW, LANES)),
        out_shape=bf((WINDOW, LANES))[0],
        scratch=[dma(len(placed))],
        name="paste",
    )(*srcs)


def gather_kernel(x_ref, o_ref, buf, sems, local):
    me = lax.axis_index("dp")
    n = BLOCK // (NAXES * ROWS) * ROWS
    spans = [(0, n), (n, n), (2 * n, BLOCK - 2 * n)]
    sent = []

    def rows(g, s):
        e = me
        for b, axis in enumerate(AXES[g]):
            if s >> b & 1:
                e = e ^ (2 << axis)
        return pl.ds(pl.multiple_of(e * BLOCK + spans[g][0], ROWS), spans[g][1])

    def send(g, s, k):
        to = me ^ 1 if k == NAXES else me ^ (2 << AXES[g][k])
        dst = o_ref.at[rows(g, s)]
        src = dst if s else x_ref.at[pl.ds(*spans[g])]
        there = s + HALF if k == NAXES else s | 1 << k
        copy = remote_copy(src, dst, sems.at[0, g, there], sems.at[1, g, there], to)
        copy.start()
        sent.append(copy)

    def landed(g, t):
        ref = o_ref.at[pl.ds(*spans[g])]
        remote_copy(ref, ref, sems.at[0, g, t], sems.at[1, g, t], me ^ 1).wait_recv()

    into = pltpu.make_async_copy(x_ref, buf, local.at[0])
    back = pltpu.make_async_copy(buf, o_ref.at[pl.ds(pl.multiple_of(me * BLOCK, ROWS), BLOCK)], local.at[1])
    into.start()
    greet()
    met()
    for k in range(4):
        for g in range(NAXES):
            send(g, 0, k)
    into.wait()
    back.start()
    for t in range(1, HALF):
        for g in range(NAXES):
            landed(g, t)
            for k in range(t.bit_length(), 4):
                send(g, t, k)
    for t in range(HALF, NDEV):
        for g in range(NAXES):
            landed(g, t)
    for copy in sent:
        copy.wait_send()
    back.wait()


def gather(block, cid):
    return pcall(
        gather_kernel,
        grid=(1,),
        in_specs=[HBM],
        out_specs=HBM,
        out_shape=bf((NDEV * BLOCK, LANES))[0],
        scratch=[pltpu.VMEM((BLOCK, LANES), BF), dma(2, NAXES, NDEV), dma(2)],
        name="gather",
        cid=cid,
    )(block)


def unflat_kernel(x_ref, o_ref, wide, *, per, skew, head_major):
    wide[:] = x_ref[:].astype(F32)
    n = (x_ref.shape[0] - SUB * (skew > 0)) // per
    for j in range(per):
        t = wide[pl.ds(j + skew, n, stride=per), :].astype(BF)
        if head_major:
            o_ref[j] = t
        else:
            o_ref[:, j * LANES : (j + 1) * LANES] = t


def unflat(flat, start, rows, per, tile, head_major=False):
    out = (per, rows, LANES) if head_major else (rows, per * LANES)
    skew = start % ROWS
    n, window = tile * per, tile * per + SUB * (skew > 0)
    source = lambda i: (pl.multiple_of(start - skew + n * i, ROWS), 0)
    return pcall(
        functools.partial(unflat_kernel, per=per, skew=skew, head_major=head_major),
        grid=(rows // tile,),
        in_specs=[pl.BlockSpec((pl.Element(window), pl.Element(LANES)), source)],
        out_specs=spec((per, tile, LANES), ".i.") if head_major else spec((tile, per * LANES), "i."),
        out_shape=bf(out)[0],
        scratch=[pltpu.VMEM((window, LANES), F32)],
        name="unflat",
    )(flat)


def rope_tables(positions):
    inv_freq = ROPE_BASE ** (-jnp.arange(HALF_LANES, dtype=F32) / HALF_LANES)
    angles = positions.astype(F32).reshape(-1)[:, None] * inv_freq
    cos, sin = jnp.cos(angles), jnp.sin(angles)
    return jnp.concatenate([cos, cos], axis=-1), jnp.concatenate([-sin, sin], axis=-1)


def adamw_apply(grad_vec, grad_norm, master_vec, mean_vec, var_vec, first_index):
    clip_scale = jnp.minimum(1.0, 1.0 / (grad_norm + 1e-6))
    clipped = grad_vec * clip_scale
    new_mean = BETA_ONE * mean_vec + (1.0 - BETA_ONE) * clipped
    new_var = BETA_TWO * var_vec + (1.0 - BETA_TWO) * clipped * clipped
    mean_hat = new_mean / (1.0 - BETA_ONE**STEP_COUNT)
    var_hat = new_var / (1.0 - BETA_TWO**STEP_COUNT)
    flat_index = first_index + lax.iota(jnp.int32, master_vec.shape[0])
    gain_two = ATTN_ROWS * LANES - DIM
    is_gain = (flat_index < DIM) | ((flat_index >= gain_two) & (flat_index < gain_two + DIM))
    decays = jnp.where(is_gain, 0.0, WEIGHT_DECAY)
    new_master = master_vec - LEARN_RATE * (mean_hat / (jnp.sqrt(var_hat) + ADAM_EPS) + decays * master_vec)
    return new_master, new_mean, new_var


def gradients(x, dy, pos_loc, attn_gain, w_query, w_key, w_value, w_out, mlp_gain, w_gate, w_up, w_down):
    wq, wk, wv, wo = w_query.transpose(1, 0, 2), w_key.reshape(DIM, -1), w_value.reshape(DIM, -1), w_out.reshape(DIM, DIM)
    gain_one, gain_two = attn_gain.astype(F32)[None], mlp_gain.astype(F32)[None]
    cos, sin = rope_tables(pos_loc)
    ids = iter(range(1, NDEV))

    normed_t, q, k, v = qkv_call(x, gain_one, wq, wk, wv, cos, sin)
    ctx, ctx_t = attn_fwd(q, k, v)
    hidden, nm, nm_t = oproj_call(ctx, wo, x, gain_two)

    prev, last, parts, gots, squares = None, [], [], [], []
    tiles = FFN // TILE
    ends = [-(-tiles * s // 3) for s in range(4)]
    for lo, hi, when in zip(ends, ends[1:], ((), PLAN["ffn"], PLAN["ffn"])):
        results = ffn_slice(nm, dy, nm_t, w_gate, w_up, w_down, lo, hi - lo, prev, last, when, parts, next(ids))
        prev, (gate, up, gate_r, up_r, *sums, sq) = results[:3], results[3:]
        gots += sums[2:]
        last, parts = [(gate, gate_r), (up, up_r)], list(zip(sums, range(2)))
        squares.append(sq)
    gated_t, d_gate, d_up = prev
    *g_down, part, got_a, got_b, sq = wgrad(
        gated_t, [(dy, 0, DIM)], DOWN_ROWS, 10, ORDER[2], next(ids), last[:1], *PLAN["wgrad"], parts
    )
    squares.append(sq)
    d_hidden, d_low, g_two, _, _, down_b, down_c, *more, sq = dn_call(
        d_gate, d_up, w_gate, w_up, hidden, dy, gain_two, last[1], g_down, part, next(ids)
    )
    gots += [got_a, got_b, *more]
    squares.append(sq)
    *g_out, _ = wgrad(ctx_t, [(d_low, 0, DIM)], BLK, 4, SAME, next(ids))
    d_context = mm_nt(d_low, wo).astype(BF)
    parts = [(down_b, 2), (down_c, 2)]
    d_q, d_k, d_v, out_part, *results, sq = attn_bwd(q, k, v, d_context, cos, sin, g_out, g_down, parts, next(ids))
    gots += results[2:]
    squares.append(sq)
    normed_t, out_slab = lax.optimization_barrier((normed_t, attn_flat(out_part, (0, PER))))
    out_all = lax.all_gather(out_slab, "dp", tiled=True)
    parts = [(p, 2) for p in results[:2]]
    rhs = [(d_q, 0, DIM), (d_k, 0, KV_DIM), (d_v, 0, KV_DIM)]
    *g_qkv, got_a, got_b, _ = wgrad(normed_t, rhs, BLK, 4, SAME, next(ids), parts=parts)
    more = [got_a, got_b]
    gate_a, up_a, gate_b, up_b, gate_c, up_c, *downs = gots + more
    slabs = collect([gate_a, gate_b, gate_c], [up_a, up_b, up_c], downs)
    d_x, _, qkv_part, told = dx_call(
        d_q, d_k, d_v, wq, wk, wv, x, gain_one, d_hidden, sum(squares), g_two, g_qkv, next(ids)
    )
    qkv_part, out_all = lax.optimization_barrier((qkv_part, out_all))
    qkv_all = lax.all_gather(attn_flat(qkv_part, (0, PER), (PER, KV_HEADS), (PER + KV_HEADS, KV_HEADS)), "dp")
    gain_sum = jnp.sum(told[:, : 2 * PER], axis=0).astype(BF)
    gain_mean = gain_sum.astype(F32) / NDEV
    grad_norm = jnp.sqrt(jnp.sum(told[:, 2 * PER :]) + jnp.sum(gain_mean * gain_mean))
    return d_x, grad_norm, gain_sum, qkv_all, out_all, slabs


def flat_block(dev, gain_sum, qkv_all, out_all, slabs):
    qn, kn = BLK * PER, BLK * KV_HEADS
    vn = SUB - PER
    head = jnp.concatenate([jnp.zeros((vn, LANES), BF), gain_sum[:PER]])
    v_at = SUB + NDEV * (qn + kn)
    start = (SHARD // LANES + vn) // SUB * SUB
    split, inside = divmod(start - v_at, kn)

    def first():
        pieces = [(0, None, 0, SUB)]
        pieces += [(1, e, 0, qn) for e in SAME] + [(1, e, qn, kn) for e in SAME]
        pieces += [(1, e, qn + kn, kn) for e in SAME[: (WINDOW - v_at) // kn]]
        return paste([head, qkv_all], pieces)

    def second():
        rear = WINDOW + start - v_at - NDEV * (kn + qn)
        tail = jnp.concatenate([gain_sum[PER:], slabs[: rear - PER]])
        pieces = [(0, split, qn + kn + inside, kn - inside)]
        pieces += [(0, e, qn + kn, kn) for e in SAME[split + 1 :]]
        pieces += [(1, None, 0, NDEV * qn), (2, None, 0, rear)]
        return paste([qkv_all, out_all, tail], pieces)

    away = [d * SHARD - (ATTN_ROWS + SLAB * (s or [0])[0]) * LANES for d, s in enumerate(FLAT_SLABS)]
    rows = [max(0, a) // (SUB * LANES) * SUB for a in away]
    rest = [a - r * LANES for a, r in zip(away, rows)]
    rest[:2] = [vn * LANES, SHARD + (vn - start) * LANES]

    def third():
        return lax.dynamic_slice(slabs, (jnp.asarray(rows, jnp.int32)[dev], 0), (WINDOW, LANES))

    window = lax.switch(jnp.minimum(dev, 2), [first, second, third])
    return lax.dynamic_slice(window.reshape(-1), (jnp.asarray(rest, jnp.int32)[dev],), (SHARD,))


def per_device(x_loc, dy_loc, pos_loc, *args):
    *weights, master_loc, mean_loc, var_loc = args
    dev = lax.axis_index("dp")
    d_x, grad_norm, *sums = gradients(x_loc.reshape(TOK, DIM), dy_loc.reshape(TOK, DIM), pos_loc, *weights)
    grad = flat_block(dev, *sums).astype(F32) / NDEV
    new_master, new_mean, new_var = adamw_apply(grad, grad_norm, master_loc, mean_loc, var_loc, dev * SHARD)

    halo = BLOCK * LANES * NDEV - NPARAM
    edge = lax.ppermute(new_master[:halo], "dp", list(zip(SAME[1:], SAME)))
    shift = BLOCK * LANES - SHARD
    block = lax.dynamic_slice(jnp.concatenate([new_master, edge]), (shift * dev,), (BLOCK * LANES,)).astype(BF)
    flat = gather(block.reshape(BLOCK, LANES), NDEV)

    new, at = [], 0
    for w in weights:
        rows = w.size // LANES
        if w.shape == (DIM, HEADS, LANES):
            new.append(unflat(flat, at, DIM, HEADS, 256, head_major=True).transpose(1, 0, 2))
        elif w.size >= DIM * DIM:
            per = w.shape[-1] // LANES
            new.append(unflat(flat, at, rows // per, per, {COLS: 384}.get(per, 896 if rows > DIM * PER else 256)).reshape(w.shape))
        else:
            new.append(flat[at : at + rows].reshape(w.shape))
        at += rows
    return (d_x.reshape(x_loc.shape), *new, new_master, new_mean, new_var, grad_norm)


def solution(mesh):
    split, same = P("dp"), P()
    in_specs = (split,) * 3 + (same,) * 9 + (split,) * 3
    out_specs = (split,) + (same,) * 9 + (split,) * 3 + (same,)
    return jax.shard_map(per_device, mesh=mesh, in_specs=in_specs, out_specs=out_specs, check_vma=False)
```

```python
import functools

import jax
import jax.numpy as jnp
import numpy as np
from jax import lax
from jax.experimental import pallas as pl
from jax.experimental.pallas import tpu as pltpu
from jax.sharding import PartitionSpec as P

NORM_EPS = 1e-5
ROPE_BASE = 10000.0
LEARN_RATE = 2e-3
BETA_ONE = 0.9
BETA_TWO = 0.95
ADAM_EPS = 1e-8
WEIGHT_DECAY = 0.1
STEP_COUNT = 100
BF = jnp.bfloat16
F32 = jnp.float32
MESH = pl.DeviceIdType.MESH
LANES = 128
SUB = 16
ROWS = SUB // 2
NAXES = 3
TILE = 256
HALF_LANES = LANES // 2
DIM = 1536
HEADS = 12
KV_HEADS = 2
GROUP = HEADS // KV_HEADS
KV_DIM = KV_HEADS * LANES
QKV_DIM = DIM + 2 * KV_DIM
FFN = 8960
SEQ = 768
TOK = 2 * SEQ
NDEV = 16
HALF = NDEV // 2
BLK = DIM // NDEV
NPARAM = 46795776
SHARD = NPARAM // NDEV
COLS = FFN // LANES
PER = DIM // LANES
ATTN_ROWS = PER * (2 + 2 * DIM) + 2 * KV_HEADS * DIM
SLAB = BLK * COLS
SLOTS = 5
DOWN_ROWS = FFN // NDEV // SLOTS
BLOCK = 22856
WINDOW = 22880
SCALE = LANES**-0.5
LOG2_E = float(np.log2(np.e))
HBM = pl.BlockSpec(memory_space=pl.ANY)

HOLDERS = "1b028a37945dc6fe" + "6745e81d9c0a2fb3" + "23b95c081da7ef46"
SLAB_DEV = [int(c, NDEV) for c in HOLDERS]
ORDER = [[SLAB_DEV[w * NDEV : (w + 1) * NDEV].index(d) for d in range(NDEV)] for w in range(3)]
SAME = list(range(NDEV))

PLAN = {
    "ffn": ("0369bb", "158abb"),
    "wgrad": ("136777",),
    "dn": ("14begg", "26fhij", "48imor", "lmoqrr"),
    "attn_bwd": ("1369bb", "247abb", "258bbb"),
    "dx": ("1245",),
}


def mm(a, b):
    return jnp.dot(a, b, preferred_element_type=F32)


def mm_nt(a, b):
    return lax.dot_general(a, b, (((1,), (1,)), ((), ())), preferred_element_type=F32)


def mm_tn(a, b):
    return lax.dot_general(a, b, (((0,), (0,)), ((), ())), preferred_element_type=F32)


def step(c):
    return int(c, 36)


def once(i):
    return pl.when(i == 0)


def row_mean(x):
    return jnp.mean(x, axis=-1, keepdims=True)


def row_sum(x):
    return jnp.sum(x, axis=-1, keepdims=True)


def inv_rms(x):
    return lax.rsqrt(row_mean(x * x) + NORM_EPS)


def spec(shape, index, first=0):
    return pl.BlockSpec(shape, lambda *g: tuple(0 if c == "." else g["ijk".index(c)] + first for c in index))


def full(shape):
    return pl.BlockSpec(shape, lambda *_: (0,) * len(shape), pipeline_mode=pl.Buffered(1))


def bf(*shapes):
    return [jax.ShapeDtypeStruct(s, BF) for s in shapes]


def f32(*shapes):
    return [jax.ShapeDtypeStruct(s, F32) for s in shapes]


def dma(*shape):
    return pltpu.SemaphoreType.DMA(shape)


def pcall(kernel, *, grid, in_specs, out_specs, out_shape, name, scratch=(), carry=(), cid=None):
    carry = list(carry or ())
    head, skip = len(in_specs), len(carry)

    def body(*refs):
        kernel(*refs[:head], *refs[head + skip :])

    remote = {} if cid is None else dict(collective_id=cid, has_side_effects=True)
    call = pl.pallas_call(
        body,
        grid=grid,
        in_specs=list(in_specs) + [HBM] * skip,
        out_specs=out_specs,
        scratch_shapes=list(scratch),
        out_shape=out_shape,
        input_output_aliases={head + j: j for j in range(skip)},
        compiler_params=pltpu.CompilerParams(vmem_limit_bytes=63 << 20, **remote),
        cost_estimate=pl.CostEstimate(flops=NPARAM * TILE, bytes_accessed=NPARAM, transcendentals=0),
        name=name,
    )
    return lambda *args: call(*args, *carry)


def flat_slabs(d):
    block = SHARD / LANES
    lo = max(0, int((d * block - ATTN_ROWS) // SLAB))
    hi = int(-(-((d + 1) * block - ATTN_ROWS) // SLAB))
    return list(range(lo, min(hi, 3 * NDEV)))


FLAT_SLABS = [flat_slabs(d) for d in range(NDEV)]


def pick(table, me):
    value = jnp.int32(table[0])
    for d in SAME[1:]:
        value = jnp.where(me == d, jnp.int32(table[d]), value)
    return value


AXES = [[(g + s) % NAXES for s in range(NAXES)] for g in range(NAXES)]
LOCAL, FINAL, NSEM = range(10, 13)


def remote_copy(src, dst, send, recv, device):
    return pltpu.make_async_remote_copy(src, dst, send, recv, device_id=(device,), device_id_type=MESH)


class Scatter:
    def __init__(self, a, out, bufs, n, width, sq, row0=0):
        self.a, self.out, self.n, self.sq, self.rows = a, out, n, sq, pl.ds(row0, n)
        self.keep, *self.got, self.sems = bufs
        chunks = width // LANES
        ends = [chunks * g // NAXES * LANES for g in range(4)]
        self.cols = [pl.ds(lo, hi - lo) for lo, hi in zip(ends, ends[1:])]
        self.me = lax.axis_index("dp")
        self.chip = self.me // 2
        self.bits = [lax.rem(self.chip // (1 << b), 2) for b in range(NAXES)]

    @staticmethod
    def scratch(n, width):
        return [pltpu.VMEM((k, n, width), BF) for k in (HALF, HALF, 4, 2, 1)] + [dma(2, NSEM)]

    def remote(self, src, dst, k, device):
        return remote_copy(src, dst, self.sems.at[0, k], self.sems.at[1, k], device)

    def whole(self, stage, g):
        ref = self.got[stage + 1].at[:, :, self.cols[g]]
        return self.remote(ref, ref, 1 + NAXES * stage + g, self.me ^ 1)

    def loads(self):
        for k, dst in enumerate((self.keep, self.got[0])):
            yield pltpu.make_async_copy(self.a[k].at[:, self.rows, :], dst, self.sems.at[k, LOCAL])

    def start(self):
        for copy in self.loads():
            copy.start()

    def block(self, g, stage, t, send):
        axes = AXES[g]
        own = self.bits[axes[stage]]
        j = (1 - own if send else own) * (1 << axes[stage])
        for s in axes[:stage]:
            j += self.bits[s] * (1 << s)
        for r, s in enumerate(axes[stage + 1 :]):
            j += ((t >> r) & 1) * (1 << s)
        return j

    def push(self, stage):
        for g, axes in enumerate(AXES):
            for t in range(4 >> stage):
                src = self.keep.at[self.block(g, stage, t, True), :, self.cols[g]]
                dst = self.got[stage + 1].at[t, :, self.cols[g]]
                self.remote(src, dst, 1 + NAXES * stage + g, self.me ^ (2 << axes[stage])).start()

    def sum_rows(self, j, src, cols):
        def body(r, _):
            sl = pl.ds(pl.multiple_of(r * SUB, SUB), SUB)
            self.keep[j, sl, cols] = self.keep[j, sl, cols] + src[sl, cols]
            return 0

        lax.fori_loop(0, self.n // SUB, body, 0)

    def first(self):
        for copy in self.loads():
            copy.wait()

        def body(j, _):
            self.sum_rows(j, self.got[0].at[j], slice(None))
            return 0

        lax.fori_loop(0, HALF, body, 0)
        self.push(0)

    def merge(self, stage):
        for g in range(NAXES):
            self.whole(stage, g).wait_recv()
            for t in range(4 >> stage):
                self.sum_rows(self.block(g, stage, t, False), self.got[stage + 1].at[t], self.cols[g])
        if stage < 2:
            self.push(stage + 1)

    def hand_over(self):
        return pltpu.make_async_copy(self.keep.at[self.chip], self.out, self.sems.at[0, FINAL])

    def last(self):
        self.merge(2)
        self.hand_over().start()

        def body(r, _):
            g = self.keep[self.chip, pl.ds(pl.multiple_of(r * SUB, SUB), SUB), :].astype(F32) * (1.0 / NDEV)
            g = g * g
            total = g[: ROWS] + g[ROWS :]
            for c in range(0, total.shape[1], LANES):
                self.sq[:] += total[:, c : c + LANES]
            return 0

        lax.fori_loop(0, self.n // SUB, body, 0)

    def finish(self):
        self.hand_over().wait()
        for stage in range(NAXES):
            for g in range(NAXES):
                self.whole(stage, g).wait_send()

    def run(self, i, at, final=NPARAM):
        stages = (self.start, self.first, *(functools.partial(self.merge, s) for s in range(2)), self.last, self.finish)
        for c, todo in zip(at, stages):
            k = min(step(c), final)
            if isinstance(i, int):
                if i == k:
                    todo()
            else:
                pl.when(i == k)(todo)

    def hand_on(self, sem):
        for k in (1, 2, 4, 8):
            pl.semaphore_signal(sem, inc=1, device_id=(self.me ^ k,), device_id_type=MESH)


class Push:
    def __init__(self, src, got, sems, weight):
        self.src, self.got, self.sems, self.weight = src, got, sems, weight
        self.me = lax.axis_index("dp")

    def each(self):
        held = [self.weight * NDEV + b for b in ORDER[self.weight]]
        for k in range(2):
            own = [([d for d in SAME if h in FLAT_SLABS[d]][k:] or [-1])[0] for h in held]
            slot = [FLAT_SLABS[d].index(h) if d >= 0 else 0 for d, h in zip(own, held)]
            to, slot = pick(own, self.me), pick(slot, self.me)
            dst, recv = self.got.at[slot], self.sems.at[1, slot]
            there = remote_copy(self.src, dst, self.sems.at[0, k], recv, jnp.maximum(to, 0))
            yield to, pltpu.make_async_copy(self.src, dst, recv), there

    def start(self):
        for to, here, there in self.each():
            pl.when(to == self.me)(here.start)
            pl.when((to >= 0) & (to != self.me))(there.start)

    def finish(self):
        for to, _, there in self.each():
            pl.when((to >= 0) & (to != self.me))(there.wait_send)
        for j in range(SLOTS):
            gets = [len(s) > j and s[j] // NDEV == self.weight for s in FLAT_SLABS]
            pl.when(pick(gets, self.me) == 1)(pltpu.make_async_copy(self.src, self.got.at[j], self.sems.at[1, j]).wait)


def push_all(refs, weights, start):
    n = len(weights)
    for j, w in enumerate(weights):
        job = Push(*refs[j::n], w)
        (job.start if start else job.finish)()


SLOT_SEMS = dma(2, SLOTS)


def push_shapes(parts):
    return bf(*((SLOTS, *p.shape) for p, _ in parts))


def push_sems(parts):
    return [SLOT_SEMS] * len(parts)


def greet():
    me = lax.axis_index("dp")
    for k in SAME[1:]:
        pl.semaphore_signal(pltpu.get_barrier_semaphore(), inc=1, device_id=(me ^ k,), device_id_type=MESH)


def met():
    pl.semaphore_wait(pltpu.get_barrier_semaphore(), NDEV - 1)


SQ_SPEC = full((ROWS, LANES))
SQ = f32((ROWS, LANES))


def blocks(pairs):
    return [g.reshape(HALF, -1, g.shape[-1]) for pair in pairs for g in pair]


def row_block(order, p, core):
    j, mine = 2 * (p % HALF), p // HALF
    return jnp.where(core == mine, order[j + 1], order[j])


def head_pair(w_ref, h):
    return jnp.concatenate([w_ref[h], w_ref[h + 1]], axis=1)


def qkv_kernel(x_ref, g_ref, wq_ref, wk_ref, wv_ref, c_ref, s_ref, nt_ref, q_ref, k_ref, v_ref):
    x = x_ref[:].astype(F32)
    inv = inv_rms(x)
    n = (x * inv * g_ref[:]).astype(BF)
    nt_ref[:] = n.T
    c, s = c_ref[:], s_ref[:]

    def rope(out, t, h):
        for j in range(2):
            u = t[:, j * LANES : (j + 1) * LANES]
            cols = slice((h + j) * LANES, (h + j + 1) * LANES)
            out[:, cols] = (u * c + pltpu.roll(u, HALF_LANES, 1) * s).astype(BF)

    for h in range(0, HEADS, 2):
        rope(q_ref, mm(n, head_pair(wq_ref, h)), h)
    rope(k_ref, mm(n, wk_ref[:]), 0)
    v_ref[:] = mm(n, wv_ref[:]).astype(BF)


def qkv_call(x, gain, wq, wk, wv, cos, sin, tile=TILE):
    r = lambda w: spec((tile, w), "i.")
    return pcall(
        qkv_kernel,
        grid=(TOK // tile,),
        in_specs=[r(DIM), full(gain.shape), full(wq.shape), full(wk.shape), full(wv.shape), r(LANES), r(LANES)],
        out_specs=[spec((DIM, tile), ".i"), r(DIM), r(KV_DIM), r(KV_DIM)],
        out_shape=bf((DIM, TOK), (TOK, DIM), (TOK, KV_DIM), (TOK, KV_DIM)),
        name="qkv",
    )(x, gain, wq, wk, wv, cos, sin)


def probs(q, k, i, bq):
    s = mm_nt(q, k[: (i + 1) * bq])
    r = lax.broadcasted_iota(jnp.int32, (bq, bq), 0)
    c = lax.broadcasted_iota(jnp.int32, (bq, bq), 1)
    d = jnp.where(r >= c, s[:, i * bq :], -1e30)
    s = jnp.concatenate([s[:, : i * bq], d], axis=1) if i else d
    e = jnp.exp2((s - jnp.max(s, axis=-1, keepdims=True)) * (SCALE * LOG2_E))
    return e * (1.0 / row_sum(e))


def head_cols(h):
    return slice(h * LANES, (h + 1) * LANES)


def attn_fwd_kernel(q_ref, k_ref, v_ref, o_ref, ot_ref, *, bq):
    k, v = k_ref[:], v_ref[:]
    for i in range(SEQ // bq):
        r = slice(i * bq, (i + 1) * bq)
        for c in map(head_cols, range(GROUP)):
            p = probs(q_ref[r, c], k, i, bq).astype(BF)
            o = mm(p, v[: (i + 1) * bq]).astype(BF)
            o_ref[r, c] = o
            ot_ref[c, r] = o.T


def attn_fwd(q, k, v, bq=384):
    hq, hk = spec((SEQ, GROUP * LANES), "ij"), spec((SEQ, LANES), "ij")
    return pcall(
        functools.partial(attn_fwd_kernel, bq=bq),
        grid=(TOK // SEQ, KV_HEADS),
        in_specs=[hq, hk, hk],
        out_specs=[hq, spec((GROUP * LANES, SEQ), "ji")],
        out_shape=bf((TOK, DIM), (DIM, TOK)),
        name="attn_fwd",
    )(q, k, v)


def attn_bwd_kernel(q_ref, k_ref, v_ref, do_ref, c_ref, s_ref, out_k, out_r, down_k, down_r, *refs, weights, bq, nh):
    nw = len(weights)
    ins, (dq_ref, dk_ref, dv_ref, out_out, down_a, down_b), refs = refs[:nw], refs[nw:][:6], refs[nw + 6 :]
    gots, (sq, dka, dva), sems, refs = refs[:nw], refs[nw:][:3], refs[nw + 3 :][:nw], refs[2 * nw + 3 :]
    pushes = (*ins, *gots, *sems)
    b, kv, group = (pl.program_id(j) for j in range(NAXES))
    steps = GROUP // nh
    i = (b * KV_HEADS + kv) * steps + group
    n = DOWN_ROWS

    @once(i)
    def _():
        sq[:] = jnp.zeros_like(sq)
        greet()

    @pl.when(i == step("1"))
    def _():
        met()
        push_all(pushes, weights, True)

    down, plan = (down_k, down_r), PLAN["attn_bwd"]
    Scatter(down, down_a, refs[:6], n, DIM, sq, 3 * n).run(i, plan[0])
    Scatter(down, down_b, refs[6:12], n, DIM, sq, 4 * n).run(i, plan[1])
    Scatter((out_k, out_r), out_out, refs[12:], BLK, DIM, sq).run(i, plan[2])
    pl.when(i == step(plan[0][-1]))(lambda: push_all(pushes, weights, False))
    k, v = k_ref[:], v_ref[:]

    @once(group)
    def _():
        dka[:] = jnp.zeros_like(dka)
        dva[:] = jnp.zeros_like(dva)

    def back(t, c, s):
        return (t * c - pltpu.roll(t, HALF_LANES, 1) * s).astype(BF)

    for i in range(SEQ // bq):
        r, w = slice(i * bq, (i + 1) * bq), (i + 1) * bq
        sides = [[], [], [], []]
        for c in map(head_cols, range(nh)):
            q, do = q_ref[r, c], do_ref[r, c]
            p = probs(q, k, i, bq)
            dp = mm_nt(do, v[:w])
            ds = (p * (dp - row_sum(dp * p)) * SCALE).astype(BF)
            dq_ref[r, c] = back(mm(ds, k[:w]), c_ref[r, :], s_ref[r, :])
            for side, value in zip(sides, (ds, q, p.astype(BF), do)):
                side.append(value)
        ds, q, p, do = (jnp.concatenate(side, axis=0) for side in sides)
        dka[:w, :] += mm_tn(ds, q)
        dva[:w, :] += mm_tn(p, do)

    @pl.when(group == steps - 1)
    def _():
        dk_ref[:] = back(dka[:], c_ref[:], s_ref[:])
        dv_ref[:] = dva[:].astype(BF)


def attn_bwd(q, k, v, do, cos, sin, g_out, g_down, parts, cid, bq=384, nh=2):
    steps = GROUP // nh
    hq = pl.BlockSpec((SEQ, nh * LANES), lambda b, kv, g: (b, kv * steps + g))
    hk = spec((SEQ, LANES), "ij")
    tb = spec((SEQ, LANES), "i.")
    down = (DOWN_ROWS, DIM)
    return pcall(
        functools.partial(attn_bwd_kernel, weights=[w for _, w in parts], bq=bq, nh=nh),
        grid=(TOK // SEQ, KV_HEADS, steps),
        in_specs=[hq, hk, hk, hq, tb, tb] + [HBM] * (4 + len(parts)),
        out_specs=[hq, hk, hk] + [HBM] * (3 + len(parts)) + [SQ_SPEC],
        out_shape=bf((TOK, DIM), k.shape, v.shape, (BLK, DIM), down, down) + push_shapes(parts) + SQ,
        scratch=[pltpu.VMEM((SEQ, LANES), F32)] * 2
        + push_sems(parts)
        + Scatter.scratch(*down) * 2
        + Scatter.scratch(BLK, DIM),
        name="attn_bwd",
        cid=cid,
    )(q, k, v, do, cos, sin, *blocks([g_out, g_down]), *[p for p, _ in parts])


def oproj_kernel(c_ref, wo_ref, x_ref, g_ref, h_ref, n_ref, nt_ref):
    h = (x_ref[:].astype(F32) + mm(c_ref[:], wo_ref[:])).astype(BF)
    h_ref[:] = h
    hw = h.astype(F32)
    inv = inv_rms(hw)
    n = (hw * inv * g_ref[:]).astype(BF)
    n_ref[:] = n
    nt_ref[:] = n.T


def oproj_call(ctx, wo, x, gain, tile=TILE):
    r = spec((tile, DIM), "i.")
    return pcall(
        oproj_kernel,
        grid=(TOK // tile,),
        in_specs=[r, full(wo.shape), r, full(gain.shape)],
        out_specs=[r, r, spec((DIM, tile), ".i")],
        out_shape=bf((TOK, DIM), (TOK, DIM), (DIM, TOK)),
        name="oproj",
    )(ctx, wo, x, gain)


def ffn_kernel(nm_h, dy_h, nt_h, wg_ref, wu_ref, wd_ref, *refs, units, at, weights, count, rc):
    nu, nw = len(units), len(weights)
    ins, refs = refs[: 2 * nu + nw], refs[2 * nu + nw :]
    (gt_ref, dg_ref, du_ref, gg_ref, gu_ref, rg_h, ru_h), refs = refs[:7], refs[7:]
    outs, (sq, nm, dy, na, nb, out, sem, core_sem), refs = refs[: nu + nw], refs[nu + nw :][:8], refs[nu + nw + 8 :]
    pushes = (*ins[2 * nu :], *outs[nu:], *refs[:nw])
    i = pl.program_id(0)
    me = lax.axis_index("dp")
    half, tile = out.shape[-2:]
    loads = [(nm_h, nm), (dy_h, dy), (nt_h, na), (nt_h, nb)]

    @once(i)
    def _():
        sq[:] = jnp.zeros_like(sq)
        for j, (src, dst) in enumerate(loads):
            if src is not nt_h:
                pltpu.make_async_copy(src, dst, sem.at[j]).start()
                continue
            for p in range(NDEV):
                b = row_block(ORDER[j - 2], p, lax.rem(me, 2))
                rows = src.at[pl.ds(pl.multiple_of(b * BLK, BLK), BLK)]
                pltpu.make_async_copy(rows, dst.at[pl.ds(p * BLK, BLK)], sem.at[j]).start()
        greet()

    jobs = [
        Scatter(ins[2 * u :][:2], outs[u], refs[nw + 6 * u :][:6], *unit, sq) for u, unit in enumerate(units)
    ]

    @once(i)
    def _():
        for j, (src, dst) in enumerate(loads):
            pltpu.make_async_copy(src, dst, sem.at[j]).wait()

    slot = lax.rem(i, 2)

    def across(w, dst, t):
        cols = dst.at[:, pl.ds(pl.multiple_of(t * tile, tile), tile)]
        slot = lax.rem(t, 2)
        return remote_copy(out.at[slot, w], cols, core_sem.at[slot, w], core_sem.at[2, w], me ^ 1)

    @pl.when(i >= 2)
    def _():
        for w, dst in enumerate((rg_h, ru_h)):
            across(w, dst, i - 2).wait_send()

    for r in range(0, TOK, rc):
        sl = pl.ds(r, rc)
        gate = mm(nm[sl, :], wg_ref[:])
        up = mm(nm[sl, :], wu_ref[:])
        dga = mm_nt(dy[sl, :], wd_ref[:])
        sig = 1.0 / (1.0 + jnp.exp(-gate))
        act = gate * sig
        gt_ref[:, sl] = (act * up).astype(BF).T
        du_ref[sl, :] = (dga * act).astype(BF)
        dg_ref[sl, :] = (dga * up * sig * (1.0 + gate * (1.0 - sig))).astype(BF)

    @once(i)
    def _():
        met()
        push_all(pushes, weights, True)

    for job, when in zip(jobs, at):
        job.run(i, when, count - 1)
    if nw:
        pl.when(i == count - 1)(lambda: push_all(pushes, weights, False))
    for w, (src, rhs, keep) in enumerate(((na, dg_ref, gg_ref), (nb, du_ref, gu_ref))):
        out[slot, w] = mm(src[:half, :], rhs[:]).astype(BF)
        keep[:] = mm(src[half:, :], rhs[:]).astype(BF)
    for w, dst in enumerate((rg_h, ru_h)):
        across(w, dst, i).start()

        @pl.when(i == count - 1)
        def _(w=w, dst=dst):
            across(w, dst, i - 1).wait_send()
            across(w, dst, i).wait_send()
            remote_copy(dst, dst, core_sem.at[0, w], core_sem.at[2, w], me ^ 1).wait_recv()


def ffn_slice(nm, dy, nt, wg, wu, wd, first, count, prev, arrays, at, parts, cid, tile=TILE, rc=TILE):
    width, half = count * tile, DIM // 2
    units = [(BLK, g.shape[-1]) for g, _ in arrays]
    nmore = len(units) + len(parts)
    col, row, grad = spec((DIM, tile), ".i", first), spec((tile, DIM), "i.", first), spec((half, tile), ".i")
    outs = bf((FFN, TOK), (TOK, FFN), (TOK, FFN), *[(half, width)] * 4, *units)
    return pcall(
        functools.partial(ffn_kernel, units=units, at=at, weights=[w for _, w in parts], count=count, rc=rc),
        grid=(count,),
        in_specs=[HBM] * 3 + [col, col, row] + [HBM] * (nmore + len(units)),
        out_specs=[row, col, col, grad, grad] + [HBM] * (2 + nmore) + [SQ_SPEC],
        out_shape=outs + push_shapes(parts) + SQ,
        scratch=[pltpu.VMEM((TOK, DIM), BF)] * 4
        + [pltpu.VMEM((2, 2, half, tile), BF), dma(4), dma(3, 2)]
        + push_sems(parts)
        + [t for u in units for t in Scatter.scratch(*u)],
        name="ffn",
        carry=prev,
        cid=cid,
    )(nm, dy, nt, wg, wu, wd, *blocks(arrays), *[p for p, _ in parts])


def wgrad_kernel(lhs_h, *refs, cols, nr, per, blk, order, units, at, weights):
    nrhs, nu, nw = len(cols), len(units), len(weights)
    nm = nu + nw
    rhs_h, ins, (keep_h, other_h, *refs) = refs[:nrhs], refs[nrhs:][: nm + nu], refs[nrhs + nm + nu :]
    outs, (sq, *refs) = refs[:nm], refs[nm:]
    me = lax.axis_index("dp")
    rhs, (lhs, out, sem_l, sem_r, sem_o), refs = refs[:nrhs], refs[nrhs:][:5], refs[nrhs + 5 :]
    pushes = (*ins[2 * nu :], *outs[nu:], *refs[:nw])
    size = per * nr
    steps = NDEV * blk // size
    ring = lhs.shape[0]

    def fetch(t):
        for j in range(per):
            p, r = divmod((t * per + j) * nr, blk)
            src = lhs_h.at[pl.ds(pl.multiple_of(row_block(order, p, lax.rem(me, 2)) * blk + r, SUB), nr)]
            pltpu.make_async_copy(src, lhs.at[t % ring, pl.ds(j * nr, nr)], sem_l.at[t % ring]).start()

    def rhs_copy(j):
        c, w = cols[j]
        return pltpu.make_async_copy(rhs_h[j].at[:, pl.ds(c, w)], rhs[j], sem_r.at[j])

    def remote(src, dst, slot):
        return remote_copy(src, dst, sem_o.at[slot], sem_o.at[2], me ^ 1)

    def out_copy(t, wait):
        src, slot, half = out.at[t % 2], t % 2, steps // 2
        if t < half:
            copy = remote(src, other_h.at[pl.ds(t * size, size)], slot)
            (copy.wait_send if wait else copy.start)()
        else:
            copy = pltpu.make_async_copy(src, keep_h.at[pl.ds((t - half) * size, size)], sem_o.at[slot])
            (copy.wait if wait else copy.start)()

    fetch(0)
    for j in range(nrhs):
        rhs_copy(j).start()
    fetch(1)
    sq[:] = jnp.zeros_like(sq)
    greet()
    jobs = [Scatter(ins[2 * u :][:2], outs[u], refs[nw + 6 * u :][:6], *unit, sq) for u, unit in enumerate(units)]
    for t in range(steps):
        if t + 2 < steps:
            fetch(t + 2)
        pltpu.make_async_copy(lhs_h.at[pl.ds(0, size)], lhs.at[t % ring], sem_l.at[t % ring]).wait()
        if t >= 2:
            out_copy(t - 2, True)
        c = 0
        for j in range(nrhs):
            if t == 0:
                rhs_copy(j).wait()
            o = mm(lhs[t % ring], rhs[j][:]).astype(BF)
            out[t % 2, :, c : c + o.shape[1]] = o
            c += o.shape[1]
        if t == 0:
            met()
            push_all(pushes, weights, True)
        out_copy(t, False)
        for job in jobs:
            job.run(t, at)
    for t in range(steps - 2, steps):
        out_copy(t, True)
    remote(other_h, other_h, 0).wait_recv()
    push_all(pushes, weights, False)


def wgrad(lhs_t, rhs, nr, per, order, cid, arrays=(), at="", parts=()):
    rows, width = lhs_t.shape[0], sum(w for _, _, w in rhs)
    units = [(BLK, g.shape[-1]) for g, _ in arrays]
    nmore = len(units) + len(parts)
    return pcall(
        functools.partial(
            wgrad_kernel,
            cols=[r[1:] for r in rhs],
            nr=nr,
            per=per,
            blk=rows // NDEV,
            order=order,
            units=units,
            at=at,
            weights=[w for _, w in parts],
        ),
        grid=(1,),
        in_specs=[HBM] * (1 + len(rhs) + nmore + len(units)),
        out_specs=[HBM] * (2 + nmore) + [SQ_SPEC],
        out_shape=bf(*[(rows // 2, width)] * 2, *units) + push_shapes(parts) + SQ,
        scratch=[pltpu.VMEM((TOK, w), BF) for _, _, w in rhs]
        + [pltpu.VMEM((3, per * nr, TOK), BF), pltpu.VMEM((2, per * nr, width), BF), dma(3), dma(len(rhs)), dma(3)]
        + push_sems(parts)
        + [t for u in units for t in Scatter.scratch(*u)],
        name="wgrad",
        cid=cid,
    )(lhs_t, *[r[0] for r in rhs], *blocks(arrays), *[p for p, _ in parts])


def norm_back(d, x, g_ref, gg_ref):
    inv = inv_rms(x)
    hat = x * inv
    gg_ref[:] += jnp.sum(d * hat, axis=0, keepdims=True)
    dg = d * g_ref[:]
    return inv * (dg - hat * row_mean(dg * hat))


def dn_kernel(dg_ref, du_ref, wg_ref, wu_ref, h_ref, dy_ref, g_ref, up_k, up_r, down_k, down_r, part_h, dh_ref, dl_ref, gg_ref, *refs, up):
    up_out, down_a, down_b, down_c, got, got_up, got_a, sq, acc, ready, psem, usem, asem, *refs = refs
    push, push_up, push_a = Push(part_h, got, psem, 0), Push(up_out, got_up, usem, 1), Push(down_a, got_a, asem, 2)
    t, k = pl.program_id(0), pl.program_id(1)
    i = t * pl.num_programs(1) + k
    n = DOWN_ROWS

    @once(i)
    def _():
        gg_ref[:] = jnp.zeros_like(gg_ref)
        sq[:] = jnp.zeros_like(sq)
        greet()

    @pl.when(i == step("1"))
    def _():
        met()
        push.start()

    plan = PLAN["dn"]
    up_h, down_h = (up_k, up_r), (down_k, down_r)
    one = Scatter(down_h, down_a, refs[6:12], n, DIM, sq)
    three = Scatter(down_h, down_c, refs[6:11] + refs[18:], n, DIM, sq, 2 * n)
    Scatter(up_h, up_out, refs[:6], *up, sq).run(i, plan[0])
    one.run(i, plan[1])
    Scatter(down_h, down_b, refs[12:18], n, DIM, sq, n).run(i, plan[2])
    pl.when(i == step(plan[1][-1]))(lambda: one.hand_on(ready))
    pl.when(i == step(plan[3][0]))(lambda: pl.semaphore_wait(ready, 4))
    three.run(i, plan[3])
    pl.when(i == step(plan[0][-1]) + 1)(push_up.start)
    pl.when(i == step(plan[1][-1]) + 1)(push_a.start)

    @pl.when(i == step("r"))
    def _():
        for job in (push, push_up, push_a):
            job.finish()


    @once(k)
    def _():
        acc[:] = jnp.zeros_like(acc)

    acc[:] += mm_nt(dg_ref[:], wg_ref[:]) + mm_nt(du_ref[:], wu_ref[:])

    @pl.when(k == pl.num_programs(1) - 1)
    def _():
        def body(r, _):
            sl = pl.ds(pl.multiple_of(r * LANES, LANES), LANES)
            o = norm_back(acc[sl, :], h_ref[sl, :].astype(F32), g_ref, gg_ref) + dy_ref[sl, :].astype(F32)
            dh_ref[sl, :] = o
            dl_ref[sl, :] = o.astype(BF)
            return 0

        lax.fori_loop(0, acc.shape[0] // LANES, body, 0)


def dn_call(dg, du, wg, wu, h, dy, gain, g_up, g_down, part, cid, tt=384, tk=1280):
    up, down = (BLK, g_up[0].shape[-1]), (DOWN_ROWS, DIM)
    act, wgt, row = spec((tt, tk), "ij"), spec((DIM, tk), ".j"), spec((tt, DIM), "i.")
    gained = spec(gain.shape, "..")
    return pcall(
        functools.partial(dn_kernel, up=up),
        grid=(TOK // tt, FFN // tk),
        in_specs=[act, act, wgt, wgt, row, row, full(gain.shape)] + [HBM] * 5,
        out_specs=[row, row, gained] + [HBM] * 7 + [SQ_SPEC],
        out_shape=f32((TOK, DIM)) + bf((TOK, DIM)) + f32(gain.shape) + bf(up, *[down] * 3, *[(SLOTS, *t) for t in (part.shape, up, down)]) + SQ,
        scratch=[pltpu.VMEM((tt, DIM), F32), pltpu.SemaphoreType.REGULAR]
        + [SLOT_SEMS] * 3
        + Scatter.scratch(*up)
        + Scatter.scratch(*down) * 2
        + Scatter.scratch(*down)[-1:],
        name="dn",
        cid=cid,
    )(dg, du, wg, wu, h, dy, gain, *blocks([g_up, g_down]), part)


def dx_kernel(
    dq_ref, dk_ref, dv_ref, wq_ref, wk_ref, wv_ref, x_ref, g_ref, dh_ref, sq_ref, g_two_ref, qkv_k, qkv_r,
    dx_ref, gg_ref, qkv_out, told_ref, sq, mine, told, tell, *refs,
):
    i = pl.program_id(0)

    @once(i)
    def _():
        gg_ref[:] = jnp.zeros_like(gg_ref)
        sq[:] = sq_ref[:]
        greet()

    pl.when(i == step("1"))(met)
    scatter = Scatter((qkv_k, qkv_r), qkv_out, refs, BLK, QKV_DIM, sq)
    scatter.run(i, *PLAN["dx"])
    d = mm_nt(dk_ref[:], wk_ref[:]) + mm_nt(dv_ref[:], wv_ref[:])
    for h in range(0, HEADS, 2):
        d += mm_nt(dq_ref[:, h * LANES : (h + 2) * LANES], head_pair(wq_ref, h))
    dx_ref[:] = (norm_back(d, x_ref[:].astype(F32), g_ref, gg_ref) + dh_ref[:]).astype(BF)

    @pl.when(i == pl.num_programs(0) - 1)
    def _():
        scatter.last()
        for row, ref in enumerate((gg_ref, g_two_ref)):
            for c in range(PER):
                mine[pl.ds(row * PER + c, 1), :] = ref[:, head_cols(c)].astype(BF).astype(F32)
        mine[2 * PER :, :] = sq[:]
        me = lax.axis_index("dp")
        copies = []
        for k in SAME[1:]:
            copies.append(remote_copy(mine, told.at[me], tell.at[0, k], tell.at[1, k], me ^ k))
            copies[-1].start()
        told[me] = mine[:]
        for copy in copies:
            copy.wait()
        told_ref[:] = told[:]
        scatter.finish()


def dx_call(dq, dk, dv, wq, wk, wv, x, gain, dh, squares, g_two, g_qkv, cid, tile=TILE):
    r = lambda w: spec((tile, w), "i.")
    told = (2 * PER + squares.shape[0], LANES)
    return pcall(
        dx_kernel,
        grid=(TOK // tile,),
        in_specs=[r(DIM), r(KV_DIM), r(KV_DIM), full(wq.shape), full(wk.shape), full(wv.shape), r(DIM), full(gain.shape)]
        + [r(DIM), SQ_SPEC, full(gain.shape), HBM, HBM],
        out_specs=[r(DIM), spec(gain.shape, ".."), HBM, full((NDEV, *told))],
        out_shape=bf((TOK, DIM)) + f32(gain.shape) + bf((BLK, QKV_DIM)) + f32((NDEV, *told)),
        scratch=[pltpu.VMEM(squares.shape, F32), pltpu.VMEM(told, F32), pltpu.VMEM((NDEV, *told), F32), dma(2, NDEV)] + Scatter.scratch(BLK, QKV_DIM),
        name="dx",
        cid=cid,
    )(dq, dk, dv, wq, wk, wv, x, gain, dh, squares, g_two, *blocks([g_qkv]))


def to_lane_rows(wide, base, per, part, col, rows):
    for j in range(part.shape[1] // LANES):
        piece = part[:, j * LANES : (j + 1) * LANES].astype(F32)
        wide[pl.ds(base + col + j, rows, stride=per), :] = piece


def attn_flat_kernel(x_ref, o_ref, wide, *, segs):
    base = 0
    for col, per in segs:
        to_lane_rows(wide, base, per, x_ref[:, col * LANES : (col + per) * LANES], 0, BLK)
        base += BLK * per
    o_ref[:] = wide[:].astype(BF)


def attn_flat(x, *segs):
    rows = x.size // LANES
    return pcall(
        functools.partial(attn_flat_kernel, segs=segs),
        grid=(1,),
        in_specs=[full(x.shape)],
        out_specs=full((rows, LANES)),
        out_shape=bf((rows, LANES))[0],
        scratch=[pltpu.VMEM((rows, LANES), F32)],
        name="attn_flat",
    )(x)


def collect_kernel(*refs, ng, nd):
    gates, ups, downs = refs[:ng], refs[ng : 2 * ng], refs[2 * ng : 2 * ng + nd]
    o_h, tall, flat, wide, out, sem = refs[2 * ng + nd :]
    me = lax.axis_index("dp")
    kinds = [[s[k] // NDEV if k < len(s) else -1 for s in FLAT_SLABS] for k in range(SLOTS)]

    def copies(k, parts, dst, axis):
        at = 0
        for p in parts:
            n = p.shape[axis]
            to = dst.at[:, pl.ds(at, n)] if axis == 2 else dst.at[pl.ds(at, n)]
            yield pltpu.make_async_copy(p.at[k], to, sem.at[0])
            at += n

    for k in range(SLOTS):
        kind = pick(kinds[k], me)
        for w, parts in enumerate((gates, ups, downs)):

            @pl.when(kind == w)
            def _(k=k, w=w, parts=parts):
                todo = list(copies(k, parts, *((tall, 1) if w == 2 else (flat, 2))))
                for c in todo:
                    c.start()
                for c in todo:
                    c.wait()

        def store(k=k):
            return pltpu.make_async_copy(out, o_h.at[pl.ds(k * SLAB, SLAB)], sem.at[1])

        @pl.when(kind == 2)
        def _():
            to_lane_rows(wide, 0, PER, tall, 0, tall.shape[0])

        @pl.when((kind == 0) | (kind == 1))
        def _():
            to_lane_rows(wide, 0, COLS, flat, 0, BLK)

        if k:
            store(k - 1).wait()
        out[:] = wide[:].astype(BF)
        store().start()
    store().wait()


def collect(gates, ups, downs):
    parts = [*gates, *ups, *downs]
    return pcall(
        functools.partial(collect_kernel, ng=len(gates), nd=len(downs)),
        grid=(1,),
        in_specs=[HBM] * len(parts),
        out_specs=HBM,
        out_shape=bf((SLOTS * SLAB, LANES))[0],
        scratch=[
            pltpu.VMEM((FFN // NDEV, DIM), BF),
            pltpu.VMEM((BLK, FFN), BF),
            pltpu.VMEM((SLAB, LANES), F32),
            pltpu.VMEM((SLAB, LANES), BF),
            dma(2),
        ],
        name="collect",
    )(*parts)


def paste_kernel(*refs, pieces):
    srcs, (o_ref, sem) = refs[:-2], refs[-2:]
    todo = []
    for s, lead, row, n, dst in pieces:
        src = srcs[s] if lead is None else srcs[s].at[lead]
        todo.append(pltpu.make_async_copy(src.at[pl.ds(row, n)], o_ref.at[pl.ds(dst, n)], sem.at[len(todo)]))
    for c in todo:
        c.start()
    for c in todo:
        c.wait()


def paste(srcs, pieces):
    placed, at = [], 0
    for p in pieces:
        placed.append((*p, at))
        at += p[-1]
    return pcall(
        functools.partial(paste_kernel, pieces=placed),
        grid=(1,),
        in_specs=[HBM] * len(srcs),
        out_specs=full((WINDOW, LANES)),
        out_shape=bf((WINDOW, LANES))[0],
        scratch=[dma(len(placed))],
        name="paste",
    )(*srcs)


def gather_kernel(x_ref, o_ref, buf, sems, local):
    me = lax.axis_index("dp")
    n = BLOCK // (NAXES * ROWS) * ROWS
    spans = [(0, n), (n, n), (2 * n, BLOCK - 2 * n)]
    sent = []

    def rows(g, s):
        e = me
        for b, axis in enumerate(AXES[g]):
            if s >> b & 1:
                e = e ^ (2 << axis)
        return pl.ds(pl.multiple_of(e * BLOCK + spans[g][0], ROWS), spans[g][1])

    def send(g, s, k):
        to = me ^ 1 if k == NAXES else me ^ (2 << AXES[g][k])
        dst = o_ref.at[rows(g, s)]
        src = dst if s else x_ref.at[pl.ds(*spans[g])]
        there = s + HALF if k == NAXES else s | 1 << k
        copy = remote_copy(src, dst, sems.at[0, g, there], sems.at[1, g, there], to)
        copy.start()
        sent.append(copy)

    def landed(g, t):
        ref = o_ref.at[pl.ds(*spans[g])]
        remote_copy(ref, ref, sems.at[0, g, t], sems.at[1, g, t], me ^ 1).wait_recv()

    into = pltpu.make_async_copy(x_ref, buf, local.at[0])
    back = pltpu.make_async_copy(buf, o_ref.at[pl.ds(pl.multiple_of(me * BLOCK, ROWS), BLOCK)], local.at[1])
    into.start()
    greet()
    met()
    for k in range(4):
        for g in range(NAXES):
            send(g, 0, k)
    into.wait()
    back.start()
    for t in range(1, HALF):
        for g in range(NAXES):
            landed(g, t)
            for k in range(t.bit_length(), 4):
                send(g, t, k)
    for t in range(HALF, NDEV):
        for g in range(NAXES):
            landed(g, t)
    for copy in sent:
        copy.wait_send()
    back.wait()


def gather(block, cid):
    return pcall(
        gather_kernel,
        grid=(1,),
        in_specs=[HBM],
        out_specs=HBM,
        out_shape=bf((NDEV * BLOCK, LANES))[0],
        scratch=[pltpu.VMEM((BLOCK, LANES), BF), dma(2, NAXES, NDEV), dma(2)],
        name="gather",
        cid=cid,
    )(block)


def unflat_kernel(x_ref, o_ref, wide, *, per, skew, head_major):
    wide[:] = x_ref[:].astype(F32)
    n = (x_ref.shape[0] - SUB * (skew > 0)) // per
    for j in range(per):
        t = wide[pl.ds(j + skew, n, stride=per), :].astype(BF)
        if head_major:
            o_ref[j] = t
        else:
            o_ref[:, j * LANES : (j + 1) * LANES] = t


def unflat(flat, start, rows, per, tile, head_major=False):
    out = (per, rows, LANES) if head_major else (rows, per * LANES)
    skew = start % ROWS
    n, window = tile * per, tile * per + SUB * (skew > 0)
    source = lambda i: (pl.multiple_of(start - skew + n * i, ROWS), 0)
    return pcall(
        functools.partial(unflat_kernel, per=per, skew=skew, head_major=head_major),
        grid=(rows // tile,),
        in_specs=[pl.BlockSpec((pl.Element(window), pl.Element(LANES)), source)],
        out_specs=spec((per, tile, LANES), ".i.") if head_major else spec((tile, per * LANES), "i."),
        out_shape=bf(out)[0],
        scratch=[pltpu.VMEM((window, LANES), F32)],
        name="unflat",
    )(flat)


def rope_tables(positions):
    inv_freq = ROPE_BASE ** (-jnp.arange(HALF_LANES, dtype=F32) / HALF_LANES)
    angles = positions.astype(F32).reshape(-1)[:, None] * inv_freq
    cos, sin = jnp.cos(angles), jnp.sin(angles)
    return jnp.concatenate([cos, cos], axis=-1), jnp.concatenate([-sin, sin], axis=-1)


def adamw_apply(grad_vec, grad_norm, master_vec, mean_vec, var_vec, first_index):
    clip_scale = jnp.minimum(1.0, 1.0 / (grad_norm + 1e-6))
    clipped = grad_vec * clip_scale
    new_mean = BETA_ONE * mean_vec + (1.0 - BETA_ONE) * clipped
    new_var = BETA_TWO * var_vec + (1.0 - BETA_TWO) * clipped * clipped
    mean_hat = new_mean / (1.0 - BETA_ONE**STEP_COUNT)
    var_hat = new_var / (1.0 - BETA_TWO**STEP_COUNT)
    flat_index = first_index + lax.iota(jnp.int32, master_vec.shape[0])
    gain_two = ATTN_ROWS * LANES - DIM
    is_gain = (flat_index < DIM) | ((flat_index >= gain_two) & (flat_index < gain_two + DIM))
    decays = jnp.where(is_gain, 0.0, WEIGHT_DECAY)
    new_master = master_vec - LEARN_RATE * (mean_hat / (jnp.sqrt(var_hat) + ADAM_EPS) + decays * master_vec)
    return new_master, new_mean, new_var


def gradients(x, dy, pos_loc, attn_gain, w_query, w_key, w_value, w_out, mlp_gain, w_gate, w_up, w_down):
    wq, wk, wv, wo = w_query.transpose(1, 0, 2), w_key.reshape(DIM, -1), w_value.reshape(DIM, -1), w_out.reshape(DIM, DIM)
    gain_one, gain_two = attn_gain.astype(F32)[None], mlp_gain.astype(F32)[None]
    cos, sin = rope_tables(pos_loc)
    ids = iter(range(1, NDEV))

    normed_t, q, k, v = qkv_call(x, gain_one, wq, wk, wv, cos, sin)
    ctx, ctx_t = attn_fwd(q, k, v)
    hidden, nm, nm_t = oproj_call(ctx, wo, x, gain_two)

    prev, last, parts, gots, squares = None, [], [], [], []
    tiles = FFN // TILE
    ends = [-(-tiles * s // 3) for s in range(4)]
    for lo, hi, when in zip(ends, ends[1:], ((), PLAN["ffn"], PLAN["ffn"])):
        results = ffn_slice(nm, dy, nm_t, w_gate, w_up, w_down, lo, hi - lo, prev, last, when, parts, next(ids))
        prev, (gate, up, gate_r, up_r, *sums, sq) = results[:3], results[3:]
        gots += sums[2:]
        last, parts = [(gate, gate_r), (up, up_r)], list(zip(sums, range(2)))
        squares.append(sq)
    gated_t, d_gate, d_up = prev
    *g_down, part, got_a, got_b, sq = wgrad(
        gated_t, [(dy, 0, DIM)], DOWN_ROWS, 10, ORDER[2], next(ids), last[:1], *PLAN["wgrad"], parts
    )
    squares.append(sq)
    d_hidden, d_low, g_two, _, _, down_b, down_c, *more, sq = dn_call(
        d_gate, d_up, w_gate, w_up, hidden, dy, gain_two, last[1], g_down, part, next(ids)
    )
    gots += [got_a, got_b, *more]
    squares.append(sq)
    *g_out, _ = wgrad(ctx_t, [(d_low, 0, DIM)], BLK, 4, SAME, next(ids))
    d_context = mm_nt(d_low, wo).astype(BF)
    parts = [(down_b, 2), (down_c, 2)]
    d_q, d_k, d_v, out_part, *results, sq = attn_bwd(q, k, v, d_context, cos, sin, g_out, g_down, parts, next(ids))
    gots += results[2:]
    squares.append(sq)
    normed_t, out_slab = lax.optimization_barrier((normed_t, attn_flat(out_part, (0, PER))))
    out_all = lax.all_gather(out_slab, "dp", tiled=True)
    parts = [(p, 2) for p in results[:2]]
    rhs = [(d_q, 0, DIM), (d_k, 0, KV_DIM), (d_v, 0, KV_DIM)]
    *g_qkv, got_a, got_b, _ = wgrad(normed_t, rhs, BLK, 4, SAME, next(ids), parts=parts)
    more = [got_a, got_b]
    gate_a, up_a, gate_b, up_b, gate_c, up_c, *downs = gots + more
    slabs = collect([gate_a, gate_b, gate_c], [up_a, up_b, up_c], downs)
    d_x, _, qkv_part, told = dx_call(
        d_q, d_k, d_v, wq, wk, wv, x, gain_one, d_hidden, sum(squares), g_two, g_qkv, next(ids)
    )
    qkv_part, out_all = lax.optimization_barrier((qkv_part, out_all))
    qkv_all = lax.all_gather(attn_flat(qkv_part, (0, PER), (PER, KV_HEADS), (PER + KV_HEADS, KV_HEADS)), "dp")
    gain_sum = jnp.sum(told[:, : 2 * PER], axis=0).astype(BF)
    gain_mean = gain_sum.astype(F32) / NDEV
    grad_norm = jnp.sqrt(jnp.sum(told[:, 2 * PER :]) + jnp.sum(gain_mean * gain_mean))
    return d_x, grad_norm, gain_sum, qkv_all, out_all, slabs


def flat_block(dev, gain_sum, qkv_all, out_all, slabs):
    qn, kn = BLK * PER, BLK * KV_HEADS
    vn = SUB - PER
    head = jnp.concatenate([jnp.zeros((vn, LANES), BF), gain_sum[:PER]])
    v_at = SUB + NDEV * (qn + kn)
    start = (SHARD // LANES + vn) // SUB * SUB
    split, inside = divmod(start - v_at, kn)

    def first():
        pieces = [(0, None, 0, SUB)]
        pieces += [(1, e, 0, qn) for e in SAME] + [(1, e, qn, kn) for e in SAME]
        pieces += [(1, e, qn + kn, kn) for e in SAME[: (WINDOW - v_at) // kn]]
        return paste([head, qkv_all], pieces)

    def second():
        rear = WINDOW + start - v_at - NDEV * (kn + qn)
        tail = jnp.concatenate([gain_sum[PER:], slabs[: rear - PER]])
        pieces = [(0, split, qn + kn + inside, kn - inside)]
        pieces += [(0, e, qn + kn, kn) for e in SAME[split + 1 :]]
        pieces += [(1, None, 0, NDEV * qn), (2, None, 0, rear)]
        return paste([qkv_all, out_all, tail], pieces)

    away = [d * SHARD - (ATTN_ROWS + SLAB * (s or [0])[0]) * LANES for d, s in enumerate(FLAT_SLABS)]
    rows = [max(0, a) // (SUB * LANES) * SUB for a in away]
    rest = [a - r * LANES for a, r in zip(away, rows)]
    rest[:2] = [vn * LANES, SHARD + (vn - start) * LANES]

    def third():
        return lax.dynamic_slice(slabs, (jnp.asarray(rows, jnp.int32)[dev], 0), (WINDOW, LANES))

    window = lax.switch(jnp.minimum(dev, 2), [first, second, third])
    return lax.dynamic_slice(window.reshape(-1), (jnp.asarray(rest, jnp.int32)[dev],), (SHARD,))


def per_device(x_loc, dy_loc, pos_loc, *args):
    *weights, master_loc, mean_loc, var_loc = args
    dev = lax.axis_index("dp")
    d_x, grad_norm, *sums = gradients(x_loc.reshape(TOK, DIM), dy_loc.reshape(TOK, DIM), pos_loc, *weights)
    grad = flat_block(dev, *sums).astype(F32) / NDEV
    new_master, new_mean, new_var = adamw_apply(grad, grad_norm, master_loc, mean_loc, var_loc, dev * SHARD)

    halo = BLOCK * LANES * NDEV - NPARAM
    edge = lax.ppermute(new_master[:halo], "dp", list(zip(SAME[1:], SAME)))
    shift = BLOCK * LANES - SHARD
    block = lax.dynamic_slice(jnp.concatenate([new_master, edge]), (shift * dev,), (BLOCK * LANES,)).astype(BF)
    flat = gather(block.reshape(BLOCK, LANES), NDEV)

    new, at = [], 0
    for w in weights:
        rows = w.size // LANES
        if w.shape == (DIM, HEADS, LANES):
            new.append(unflat(flat, at, DIM, HEADS, 512, head_major=True).transpose(1, 0, 2))
        elif w.size >= DIM * DIM:
            per = w.shape[-1] // LANES
            new.append(unflat(flat, at, rows // per, per, {COLS: 384}.get(per, 896 if rows > DIM * PER else 512)).reshape(w.shape))
        else:
            new.append(flat[at : at + rows].reshape(w.shape))
        at += rows
    return (d_x.reshape(x_loc.shape), *new, new_master, new_mean, new_var, grad_norm)


def solution(mesh):
    split, same = P("dp"), P()
    in_specs = (split,) * 3 + (same,) * 9 + (split,) * 3
    out_specs = (split,) + (same,) * 9 + (split,) * 3 + (same,)
    return jax.shard_map(per_device, mesh=mesh, in_specs=in_specs, out_specs=out_specs, check_vma=False)
```
